32 devices in a mesh: groups: 2 (over x), blk: 16 (over z, y, core).
Axes of the slice: x: 2, y: 2, z: 4, core: 2. Of those that a mesh axis runs over, the one named last changes fastest.
Arguments:
- queries: bfloat16 [1024, 8192], P('groups', 'blk'), parts along dimension 0, may hold values from -41 to 41
- prefix_kv: bfloat16 [32, 64, 8, 256], P(('groups', 'blk')), parts along dimension 0, may hold values from -6 to 6
- page_counts: int32 [8], P('groups'), parts along dimension 0, may hold values from 1 to 8, 16 in all
- request_prefix: int32 [1024, 1], P(('groups', 'blk')), parts along dimension 0, may hold values from 0 to 3
- suffix_kv: bfloat16 [1024, 64, 8, 256], P(('groups', 'blk')), parts along dimension 0, may hold values from -6 to 6
- suffix_len: int32 [1024], P(('groups', 'blk')), parts along dimension 0, may hold values from 2 to 64, as said below
Outputs:
- attended: bfloat16 [1024, 8192], P('groups', 'blk'), parts along dimension 0
The draws below stay inside these ranges and needn't reach their ends.
There are 2 independent parts, one for each index of `groups`. The reference program is written for one: setup_inputs(seed, part) draws one part's arguments, and reference() takes and returns one part's arrays. A program takes and returns all parts, laid end to end along the dimension named above; each array names one. Nothing has to cross between parts.
Inputs may be any that keep to these rules, and one draw needn't show every extreme that they name: `page_counts`: the counts sum to 16; the largest is exactly half of 16. `request_prefix`: every prefix is named by some request. `suffix_len`: the requests of one device (aligned blocks of 32) include one with 64 live positions.
All inputs are finite; a program needn't handle non-finite values.
Results may differ from the reference program's by a relative error of at most 0.013.
Values may be sent and summed in bfloat16 or wider, within the bound.
A program may use at most 64 MiB of HBM per device.

```python
import math
import jax
import jax.numpy as jnp
import numpy as np
from jax import lax

NH = 64
KVH = 8
HD = 128
PAGE = 64
NPREF = 4
REQ_DEV = 32
SUF = 64
PAGES = 16
REQ = 512


def cache_draw(key):
    base_key = jax.random.fold_in(key, 41)
    cache = jnp.clip(jax.random.normal(base_key, (REQ, SUF, KVH, 2 * HD), jnp.float32), -6.0, 6.0)
    return cache


def draw_suffix_kv(key, part):
    cache = cache_draw(key)
    return cache.astype(jnp.bfloat16)


def draw_queries(key, part):
    base_key = jax.random.fold_in(key, 61)
    rows_query = jnp.clip(2.0 * jax.random.normal(base_key, (REQ, NH * HD), jnp.float32), -12.0, 12.0)
    return rows_query.astype(jnp.bfloat16)


def draw_suffix_len(key, part):
    lengths = jax.random.randint(jax.random.fold_in(key, 31), (REQ,), 2, SUF + 1)
    chosen = jax.random.randint(jax.random.fold_in(key, 32), (REQ // REQ_DEV,), 0, REQ_DEV)
    filled = jnp.arange(REQ, dtype=jnp.int32) % REQ_DEV == jnp.repeat(chosen, REQ_DEV)
    return jnp.where(filled, SUF, lengths).astype(jnp.int32)


def level_of(stream_key, extent, cuts, low, top_value):
    def one(axis_at, shards_of):
        steps = jax.random.uniform(jax.random.fold_in(jax.random.fold_in(stream_key, 6), axis_at), (shards_of,), jnp.float32, low / len(cuts), top_value / len(cuts))
        return jnp.repeat(jnp.exp(steps), extent[axis_at] // shards_of).reshape((-1,) + (1,) * (len(extent) - axis_at - 1))

    level = one(*cuts[0])
    for cut in cuts[1:]:
        level = level * one(*cut)
    return level


def picks_of(key, rows, amount, top, lift):
    order = jax.random.permutation(jax.random.fold_in(key, 1), amount)
    boost = order
    for power in range(3):
        boost = boost * boost // amount
    boost = boost * lift // amount
    tickets = jax.random.randint(jax.random.fold_in(key, 2), (rows, amount), 0, 4096) + boost
    holders = jax.random.permutation(jax.random.fold_in(key, 3), rows)[jnp.arange(amount) % rows]
    tickets = jnp.where(jnp.arange(rows)[:, None] == holders[None, :], 1 << 14, tickets)
    merit = tickets * amount + jnp.arange(amount)
    return lax.top_k(merit.astype(jnp.int32), top)[1].astype(jnp.int32)


def length_profile(number_of, total, most, skew):
    weights = [(1 << 20) // math.isqrt(grade ** skew) + 1 for grade in range(2, number_of + 1)]
    surplus, given = total - most - (number_of - 1), [1] * (number_of - 1)
    while surplus > 0:
        candidates = [i for i in range(number_of - 1) if given[i] < most]
        pool, left = sum([weights[i] for i in candidates]), surplus
        for i in candidates:
            addition = min(most - given[i], max(1, left * weights[i] // pool), surplus)
            given[i] = given[i] + addition
            surplus = surplus - addition
    return np.array([most] + given)


def uneven_parts(own_key, number_of, total, bound, lean):
    if number_of == 2:
        one = jax.random.randint(own_key, (), max(1, total - bound), min(bound, total - 1) + 1)
        return jnp.stack([one, total - one])
    sizes = jnp.asarray(length_profile(number_of, total, bound, lean), jnp.int32)
    couples = (number_of - 1) // 2
    source_of, taker = sizes[1:1 + 2 * couples:2], sizes[2:2 + 2 * couples:2]
    slack = jnp.minimum(source_of - 1, bound - taker)
    passed = jax.random.randint(jax.random.fold_in(own_key, 1), (couples,), 0, 1 << 20) % (slack + 1)
    sizes = sizes.at[1:1 + 2 * couples:2].set(source_of - passed).at[2:2 + 2 * couples:2].set(taker + passed)
    return sizes[jax.random.permutation(jax.random.fold_in(own_key, 2), number_of)]


def scatter_about(key, extent, scale, bound, shards=(), kind=jnp.bfloat16):
    values = jax.random.normal(key, extent, jnp.float32) * scale
    if len(shards) > 0:
        values = level_of(key, extent, shards, -0.22, 0.18) * values
    return jnp.clip(values, min=-bound, max=bound).astype(kind)


def setup_inputs(seed: int = 0, part: int = 0) -> dict:
    splits = jax.random.split(jax.random.key(seed), 7)
    part_splits = jax.random.split(jax.random.fold_in(splits[6], part), 7)
    return {
        "queries": draw_queries(jax.random.fold_in(jax.random.fold_in(splits[6], part), 71), part),
        "prefix_kv": scatter_about(part_splits[1], (PAGES, PAGE, KVH, 2 * HD), 1.0, 6.0, ((0, 16),)),
        "page_counts": uneven_parts(part_splits[2], NPREF, PAGES, PAGES // 2, 2).astype(jnp.int32),
        "request_prefix": picks_of(part_splits[3], REQ, NPREF, 1, 4096),
        "suffix_kv": draw_suffix_kv(jax.random.fold_in(jax.random.fold_in(splits[6], part), 71), part),
        "suffix_len": draw_suffix_len(jax.random.fold_in(jax.random.fold_in(splits[6], part), 71), part),
    }


neg_large = -1.0e30


def reference(queries, prefix_kv, page_counts, request_prefix, suffix_kv, suffix_len):
    group_size = NH // KVH
    score_scale = HD ** -0.5
    page_ends = jnp.cumsum(page_counts)
    page_index = jnp.arange(PAGES, dtype=jnp.int32)
    page_owner = jnp.sum((page_index[:, None] >= page_ends[None, :]).astype(jnp.int32), axis=1)
    token_owner = jnp.repeat(page_owner, PAGE)
    pooled = prefix_kv.reshape(PAGES * PAGE, KVH, 2 * HD).astype(jnp.float32)
    pool_keys = pooled[:, :, :HD]
    pool_values = pooled[:, :, HD:]
    block_count = REQ // REQ_DEV

    def one_block(pieces):
        rows_query, rows_owner, rows_cache, rows_length = pieces
        query_full = rows_query.astype(jnp.float32).reshape(REQ_DEV, KVH, group_size, HD)
        cache_full = rows_cache.astype(jnp.float32)
        prefix_scores = jnp.einsum("rkgd,tkd->rkgt", query_full, pool_keys) * score_scale
        suffix_scores = jnp.einsum("rkgd,rtkd->rkgt", query_full, cache_full[..., :HD]) * score_scale
        prefix_live = (rows_owner[:, None] == token_owner[None, :])[:, None, None, :]
        suffix_live = (jnp.arange(SUF, dtype=jnp.int32)[None, :] < rows_length[:, None])[:, None, None, :]
        prefix_scores = jnp.where(prefix_live, prefix_scores, neg_large)
        suffix_scores = jnp.where(suffix_live, suffix_scores, neg_large)
        top_score = jnp.maximum(jnp.max(prefix_scores, axis=-1), jnp.max(suffix_scores, axis=-1))
        prefix_weight = jnp.where(prefix_live, jnp.exp(prefix_scores - top_score[..., None]), 0.0)
        suffix_weight = jnp.where(suffix_live, jnp.exp(suffix_scores - top_score[..., None]), 0.0)
        weight_sum = jnp.sum(prefix_weight, axis=-1) + jnp.sum(suffix_weight, axis=-1)
        prefix_round = lax.optimization_barrier(prefix_weight.astype(jnp.bfloat16)).astype(jnp.float32)
        suffix_round = lax.optimization_barrier(suffix_weight.astype(jnp.bfloat16)).astype(jnp.float32)
        mixed_sum = jnp.einsum("rkgt,tkd->rkgd", prefix_round, pool_values)
        mixed_sum = mixed_sum + jnp.einsum("rkgt,rtkd->rkgd", suffix_round, cache_full[..., HD:])
        result = (mixed_sum / weight_sum[..., None]).astype(jnp.bfloat16)
        return result.reshape(REQ_DEV, NH * HD)

    outputs = lax.map(one_block, (
        queries.reshape(block_count, REQ_DEV, NH * HD),
        request_prefix.reshape(block_count, REQ_DEV),
        suffix_kv.reshape(block_count, REQ_DEV, SUF, KVH, 2 * HD),
        suffix_len.reshape(block_count, REQ_DEV)))
    return outputs.reshape(REQ, NH * HD)
```

```python
import functools
import math

import jax
import jax.numpy as jnp
from jax import lax
from jax.experimental import pallas as pl
from jax.experimental.pallas import tpu as pltpu
from jax.sharding import PartitionSpec as P

neg_large = -1e30


def div(x, k):
    return jnp.right_shift(x, k.bit_length() - 1) if k & (k - 1) == 0 else x // k


def mod(x, k):
    return jnp.bitwise_and(x, k - 1) if k & (k - 1) == 0 else lax.rem(x, k)


MESH = pl.DeviceIdType.MESH
CHUNKS = 2
UNROLL = 4
LANES = 128
PREFIX_KI = 256
VMEM_MIB = 56
LOG2E = math.log2(math.e)


def kernel(
    n, q_hbm, kv_hbm, rp_ref, pc_ref, suf_ref, len_ref, out_ref,
    q_ref, kv_ref, home, order, back, qrecv, qperm, operm, retsrc, retrecv, pool, suf, own_recv,
    own_col, stats_src, stats_recv, mix, second_factor, top, total,
    q_send, q_recv_sem, own_send, own_recv_sem, kv_send, kv_recv, fw_send,
    ret_send, ret_recv, st_send, st_recv, suf_sem, in_sem,
):
    me = lax.axis_index("blk")
    partner = me + 1 - 2 * lax.rem(me, 2)
    rows_all, width = q_ref.shape
    req_dev = rows_all // n
    part = req_dev // CHUNKS
    kv_heads, page_len, kv_width = home.shape
    head_dim = kv_width // 2
    per_dev = width // head_dim
    heads = per_dev * n
    group_size = heads // kv_heads
    share = n // kv_heads
    cols = suf_ref.shape[1]
    scale = head_dim ** -0.5 * LOG2E
    power = n & (n - 1) == 0

    def iota(shape, dim):
        return lax.broadcasted_iota(jnp.int32, shape, dim)

    barrier = pltpu.get_barrier_semaphore()

    @pl.loop(1, n)
    def _(k):
        pl.semaphore_signal(
            barrier, inc=1, device_id={"blk": lax.rem(me + k, n)}, device_id_type=MESH
        )

    q_in = pltpu.make_async_copy(q_hbm, q_ref, in_sem.at[0])
    kv_in = pltpu.make_async_copy(kv_hbm, kv_ref, in_sem.at[1])
    q_in.start()
    kv_in.start()

    def suf_copy(r):
        return pltpu.make_async_copy(suf_ref.at[r], suf.at[r], suf_sem.at[r])

    @pl.loop(0, req_dev)
    def _(r):
        suf_copy(r).start()

    def send(src, dst, s_sem, r_sem, peer):
        return pltpu.make_async_remote_copy(
            src_ref=src, dst_ref=dst, send_sem=s_sem, recv_sem=r_sem,
            device_id={"blk": peer}, device_id_type=MESH,
        )

    def peer_of(j):
        return jnp.bitwise_xor(me, j + 1) if power else lax.rem(me + j + 1, n)

    def source_of(j):
        return jnp.bitwise_xor(me, j + 1) if power else lax.rem(me + n - j - 1, n)

    def q_copy(c, slot, peer):
        rows = pl.ds(pl.multiple_of(peer * req_dev + c * part, part), part)
        return send(q_ref.at[rows], qrecv.at[c, slot], q_send.at[c], q_recv_sem.at[c], peer)

    def q_all(c):
        some = qrecv.at[c, pl.ds(0, n - 1)]
        return send(some, some, q_send.at[c], q_recv_sem.at[c], partner)

    def own_copy(slot, peer):
        return send(rp_ref, own_recv.at[slot], own_send, own_recv_sem, peer)

    def own_all():
        some = own_recv.at[pl.ds(0, n - 1)]
        return send(some, some, own_send, own_recv_sem, partner)

    def kv_copy(slot, peer):
        return send(home.at[peer // share], pool.at[slot], kv_send, kv_recv.at[slot], peer)

    def kv_all():
        some = pool.at[pl.ds(0, n // 2 - 1)]
        return send(some, some, kv_send, kv_recv.at[0], partner)

    def fw_copy(slot):
        return send(pool.at[slot], pool.at[slot], fw_send, kv_recv.at[slot], partner)

    def fw_own():
        return send(home.at[me // share], pool.at[me], fw_send, kv_recv.at[me], partner)

    def fw_all():
        some = pool.at[pl.ds(0, n // 2)]
        return send(some, some, fw_send, kv_recv.at[0], partner)

    def ret_copy(c, slot, peer):
        return send(
            retsrc.at[c, peer], retrecv.at[c, slot], ret_send.at[c], ret_recv.at[c, slot], peer
        )

    def ret_all(c):
        some = retsrc.at[c, pl.ds(0, n - 1)]
        return send(some, some, ret_send.at[c], ret_recv.at[c, 0], partner)

    def st_copy(slot, peer):
        return send(stats_src.at[peer], stats_recv.at[slot], st_send, st_recv, peer)

    def st_all():
        some = stats_recv.at[pl.ds(0, n - 1)]
        return send(some, some, st_send, st_recv, partner)

    q_in.wait()
    pl.semaphore_wait(barrier, n - 1)

    for c in range(CHUNKS):

        @pl.loop(0, n - 1)
        def _(j, c=c):
            q_copy(c, me, peer_of(j)).start()

        if c == 0:

            @pl.loop(0, n - 1)
            def _(j):
                own_copy(me, peer_of(j)).start()

    for c in range(CHUNKS):
        qrecv[c, me] = q_ref[pl.ds(pl.multiple_of(me * req_dev + c * part, part), part)]
    own_recv[me] = rp_ref[...]

    kv_in.wait()
    entries = kv_heads * page_len
    entry, source = iota((entries, entries), 0), iota((entries, entries), 1)
    turn = jnp.where(
        source == mod(entry, page_len) * kv_heads + div(entry, page_len), 1.0, 0.0
    ).astype(jnp.bfloat16)
    turned = jnp.dot(turn, kv_ref[...], preferred_element_type=jnp.float32)
    home[...] = turned.astype(jnp.bfloat16).reshape(home.shape)
    pool[me] = home[me // share]

    @pl.loop(1, n // 2)
    def _(j):
        kv_copy(me, lax.rem(me + 2 * j, n)).start()

    fw_own().start()

    size = part * n
    row_id, col_id = iota((size, size), 0), iota((size, size), 1)
    order[...] = jnp.where(
        col_id == mod(row_id, n) * part + div(row_id, n), 1.0, 0.0
    ).astype(jnp.bfloat16)
    back[...] = jnp.where(
        col_id == mod(row_id, part) * n + div(row_id, part), 1.0, 0.0
    ).astype(jnp.bfloat16)
    stacked = iota((per_dev * n, cols), 0)
    head_of_row = mod(stacked, n) * per_dev + div(stacked, n)
    column = iota((per_dev * n, cols), 1)
    own_kv = div(head_of_row, group_size) == mod(column, kv_heads)
    position = jnp.where(own_kv, div(column, kv_heads), cols)
    lane = iota((n, LANES), 1)

    seen = jnp.zeros((n, LANES), jnp.float32)
    for c in range(CHUNKS):
        q_all(c).wait_recv()
        qperm[...] = jnp.dot(
            order[...], qrecv[c].reshape(size, width), preferred_element_type=jnp.float32
        ).astype(jnp.bfloat16)

        def some_requests(step, seen, c=c):
            ids = [step * UNROLL + u for u in range(UNROLL)]
            all_scores = []
            for local in ids:
                r = c * part + local
                suf_copy(r).wait()
                rows = pl.ds(pl.multiple_of(local * n, n), n)
                qr = jnp.concatenate(
                    [qperm[rows, h * head_dim:(h + 1) * head_dim] for h in range(per_dev)], axis=0
                )
                all_scores.append(lax.dot_general(
                    qr, suf[r, :, :head_dim], (((1,), (1,)), ((), ())),
                    preferred_element_type=jnp.float32,
                ))
            for local, scores in zip(ids, all_scores):
                r = c * part + local
                rows = pl.ds(pl.multiple_of(local * n, n), n)
                scores = jnp.where(position < len_ref[r], scores, neg_large)
                top_score = jnp.max(scores, axis=1, keepdims=True)
                weight = jnp.exp2((scores - top_score) * scale)
                weight_sum = jnp.sum(weight, axis=1, keepdims=True)
                mixed = jnp.dot(
                    weight.astype(jnp.bfloat16), suf[r, :, head_dim:],
                    preferred_element_type=jnp.float32,
                )
                result = (mixed * (1.0 / weight_sum)).astype(jnp.bfloat16)
                level = top_score * scale + jnp.log(weight_sum) * LOG2E
                for h in range(per_dev):
                    operm[rows, h * head_dim:(h + 1) * head_dim] = result[h * n:(h + 1) * n]
                    seen = jnp.where(
                        lane == h * req_dev + r, level[h * n:(h + 1) * n], seen
                    )
            return seen

        seen = lax.fori_loop(0, part // UNROLL, some_requests, seen)
        if c == CHUNKS - 1:
            for p in range(n):
                stats_src[p] = seen[p:p + 1, :]

            @pl.loop(0, n - 1)
            def _(j):
                st_copy(me, peer_of(j)).start()

        returned = jnp.dot(back[...], operm[...], preferred_element_type=jnp.float32)
        retsrc[c] = returned.astype(jnp.bfloat16).reshape(n, part, width)

        @pl.loop(0, n - 1)
        def _(j, c=c):
            ret_copy(c, me, peer_of(j)).start()

        retrecv[c, me] = retsrc[c, me]
        if c == 0:
            own_all().wait_recv()
            eye = iota((req_dev, req_dev), 0) == iota((req_dev, req_dev), 1)
            for s in range(n):
                own_col[s * req_dev:(s + 1) * req_dev] = jnp.sum(
                    jnp.where(eye, own_recv[s].astype(jnp.float32), 0.0), axis=1, keepdims=True
                )
    stats_recv[me] = stats_src[me]

    @pl.loop(1, n // 2)
    def _(j):
        slot = lax.rem(me + 2 * j, n)
        kv_copy(slot, me).wait_recv()
        fw_copy(slot).start()

    @pl.loop(0, n // 2)
    def _(j):
        slot = lax.rem(partner + 2 * j, n)
        fw_copy(slot).wait_recv()

    tokens = n * page_len
    page = div(iota((1, tokens), 1), page_len)
    token_owner = jnp.zeros((1, tokens), jnp.float32)
    end = jnp.int32(0)
    for i in range(pc_ref.shape[0]):
        end = end + pc_ref[i]
        token_owner = token_owner + jnp.where(page >= end, 1.0, 0.0)

    block = max(32, min(rows_all, PREFIX_KI * 1024 // tokens))

    @pl.loop(0, rows_all // block)
    def _(b):
        rows = pl.ds(pl.multiple_of(b * block, block), block)
        live = own_col[rows] == token_owner
        keys = pool[:, :, :head_dim].reshape(tokens, head_dim)
        values = pool[:, :, head_dim:].reshape(tokens, head_dim)
        for h in range(per_dev):
            scores = lax.dot_general(
                q_ref[rows, h * head_dim:(h + 1) * head_dim], keys, (((1,), (1,)), ((), ())),
                preferred_element_type=jnp.float32,
            )
            scores = jnp.where(live, scores, neg_large)
            top_score = jnp.max(scores, axis=1, keepdims=True)
            weight = jnp.exp2((scores - top_score) * scale)
            top[h, rows] = top_score * scale
            total[h, rows] = jnp.sum(weight, axis=1, keepdims=True)
            mix[rows, h * head_dim:(h + 1) * head_dim] = jnp.dot(
                weight.astype(jnp.bfloat16), values, preferred_element_type=jnp.float32
            )

    for c in range(CHUNKS):
        q_all(c).wait_send()
    own_all().wait_send()
    kv_all().wait_send()
    fw_all().wait_send()

    st_all().wait_recv()
    sub, lan = iota((req_dev, LANES), 0), iota((req_dev, LANES), 1)

    @pl.loop(0, n // 2)
    def _(step):
        for u in range(2):
            s = step * 2 + u
            rows = pl.ds(pl.multiple_of(s * req_dev, req_dev), req_dev)
            row = stats_recv[s]
            for h in range(per_dev):
                span = slice(h * head_dim, (h + 1) * head_dim)
                level = jnp.sum(
                    jnp.where(lan == h * req_dev + sub, row, 0.0), axis=1, keepdims=True
                )
                top_first = top[h, rows]
                top_score = jnp.maximum(level, top_first)
                factor_second = jnp.exp2(level - top_score)
                factor_first = jnp.exp2(top_first - top_score)
                inverse = 1.0 / (total[h, rows] * factor_first + factor_second)
                mix[rows, span] = mix[rows, span] * (factor_first * inverse)
                second_factor[rows, span] = jnp.broadcast_to(
                    factor_second * inverse, (req_dev, head_dim)
                )

    def gather_in(c, s):
        rows = pl.ds(pl.multiple_of(s * req_dev + c * part, part), part)
        second = retrecv[c, s].astype(jnp.float32)
        out_ref[rows, :] = (mix[rows, :] + second * second_factor[rows, :]).astype(out_ref.dtype)

    for c in range(CHUNKS):
        gather_in(c, me)

        @pl.loop(0, n - 1)
        def _(j, c=c):
            slot = source_of(j)
            ret_copy(c, slot, me).wait_recv()
            gather_in(c, slot)

    st_all().wait_send()
    for c in range(CHUNKS):
        ret_all(c).wait_send()


def body(queries, prefix_kv, page_counts, request_prefix, suffix_kv, suffix_len):
    n = lax.axis_size("blk")
    rows_all, width = queries.shape
    req_dev, suf_len, kv_heads, kv_width = suffix_kv.shape
    head_dim = kv_width // 2
    per_dev = width // head_dim
    page_len = prefix_kv.shape[1]
    part = req_dev // CHUNKS
    page = prefix_kv.reshape(page_len * kv_heads, kv_width)
    cache = suffix_kv.reshape(req_dev, suf_len * kv_heads, kv_width)
    bf16, f32, i32 = jnp.bfloat16, jnp.float32, jnp.int32
    dma = pltpu.SemaphoreType.DMA
    vmem = pl.BlockSpec(memory_space=pltpu.VMEM)
    smem = pl.BlockSpec(memory_space=pltpu.SMEM)
    anywhere = pl.BlockSpec(memory_space=pl.ANY)
    return pl.pallas_call(
        functools.partial(kernel, n),
        out_shape=pltpu.VMEM((rows_all, width), bf16),
        in_specs=[anywhere, anywhere, vmem, smem, anywhere, smem],
        out_specs=vmem,
        scratch_shapes=[
            pltpu.VMEM((rows_all, width), bf16),
            pltpu.VMEM((page_len * kv_heads, kv_width), bf16),
            pltpu.VMEM((kv_heads, page_len, kv_width), bf16),
            pltpu.VMEM((part * n, part * n), bf16),
            pltpu.VMEM((part * n, part * n), bf16),
            pltpu.VMEM((CHUNKS, n, part, width), bf16),
            pltpu.VMEM((part * n, width), bf16),
            pltpu.VMEM((part * n, width), bf16),
            pltpu.VMEM((CHUNKS, n, part, width), bf16),
            pltpu.VMEM((CHUNKS, n, part, width), bf16),
            pltpu.VMEM((n, page_len, kv_width), bf16),
            pltpu.VMEM((req_dev, suf_len * kv_heads, kv_width), bf16),
            pltpu.VMEM((n, 1, req_dev), i32),
            pltpu.VMEM((rows_all, 1), f32),
            pltpu.VMEM((n, 1, LANES), f32),
            pltpu.VMEM((n, 1, LANES), f32),
            pltpu.VMEM((rows_all, width), f32),
            pltpu.VMEM((rows_all, width), f32),
            pltpu.VMEM((per_dev, rows_all, 1), f32),
            pltpu.VMEM((per_dev, rows_all, 1), f32),
            dma((CHUNKS,)), dma((CHUNKS,)), dma, dma, dma, dma((n,)), dma,
            dma((CHUNKS,)), dma((CHUNKS, n)), dma, dma, dma((req_dev,)), dma((2,)),
        ],
        compiler_params=pltpu.CompilerParams(
            collective_id=0, has_side_effects=True, vmem_limit_bytes=VMEM_MIB * 1024 * 1024
        ),
    )(queries, page, request_prefix.T, page_counts, cache, suffix_len)


def solution(mesh):
    in_specs = (
        P("groups", "blk"),
        P(("groups", "blk"), None, None, None),
        P("groups"),
        P(("groups", "blk"), None),
        P(("groups", "blk"), None, None, None),
        P(("groups", "blk")),
    )
    out_specs = P("groups", "blk")
    return jax.shard_map(body, mesh=mesh, in_specs=in_specs, out_specs=out_specs, check_vma=False)
```

```python
import functools
import math

import jax
import jax.numpy as jnp
from jax import lax
from jax.experimental import pallas as pl
from jax.experimental.pallas import tpu as pltpu
from jax.sharding import PartitionSpec as P

neg_large = -1e30


def div(x, k):
    return jnp.right_shift(x, k.bit_length() - 1) if k & (k - 1) == 0 else x // k


def mod(x, k):
    return jnp.bitwise_and(x, k - 1) if k & (k - 1) == 0 else lax.rem(x, k)


MESH = pl.DeviceIdType.MESH
CHUNKS = 2
UNROLL = 8
LANES = 128
PREFIX_KI = 256
VMEM_MIB = 56
LOG2E = math.log2(math.e)


def plane_of(n):
    bits = n.bit_length() - 1
    return 1 << (bits + 1) // 2 if n & (n - 1) == 0 else 1


def kernel(
    n, q_hbm, kv_hbm, rp_ref, pc_ref, suf_ref, len_ref, out_ref,
    q_ref, kv_ref, home, order, back, qrecv, qperm, operm, retsrc, retrecv, pool, suf, own_recv,
    own_col, stats_src, stats_recv, mix, second_factor, top, total,
    q_send, q_recv_sem, own_send, own_recv_sem, kv_send, kv_recv, fw_send,
    ret_send, ret_recv, st_send, st_recv, suf_sem, in_sem, from_below, from_above,
):
    me = lax.axis_index("blk")
    partner = me + 1 - 2 * lax.rem(me, 2)
    rows_all, width = q_ref.shape
    req_dev = rows_all // n
    part = req_dev // CHUNKS
    kv_heads, page_len, kv_width = home.shape
    head_dim = kv_width // 2
    per_dev = width // head_dim
    heads = per_dev * n
    group_size = heads // kv_heads
    share = n // kv_heads
    cols = suf_ref.shape[1]
    scale = head_dim ** -0.5 * LOG2E
    power = n & (n - 1) == 0

    def iota(shape, dim):
        return lax.broadcasted_iota(jnp.int32, shape, dim)

    def signal(sem, peer):
        pl.semaphore_signal(sem, inc=1, device_id={"blk": peer}, device_id_type=MESH)

    barrier = pltpu.get_barrier_semaphore()
    side = plane_of(n)
    planes = n // side
    plane, spot = div(me, side), mod(me, side)
    has_up, has_down = plane + 1 < planes, plane > 0
    up, down = lax.rem(me + side, n), lax.rem(me + n - side, n)

    @pl.when(has_up)
    def _():
        signal(barrier, up)

    @pl.when(has_down)
    def _():
        signal(barrier, down)

    @pl.loop(1, side)
    def _(k):
        signal(barrier, plane * side + jnp.bitwise_xor(spot, k))

    q_in = pltpu.make_async_copy(q_hbm, q_ref, in_sem.at[0])
    kv_in = pltpu.make_async_copy(kv_hbm, kv_ref, in_sem.at[1])
    q_in.start()
    kv_in.start()

    def suf_copy(r):
        return pltpu.make_async_copy(suf_ref.at[r], suf.at[r], suf_sem.at[r])

    @pl.loop(0, req_dev)
    def _(r):
        suf_copy(r).start()

    def send(src, dst, s_sem, r_sem, peer):
        return pltpu.make_async_remote_copy(
            src_ref=src, dst_ref=dst, send_sem=s_sem, recv_sem=r_sem,
            device_id={"blk": peer}, device_id_type=MESH,
        )

    def peer_of(j):
        return jnp.bitwise_xor(me, j + 1) if power else lax.rem(me + j + 1, n)

    def source_of(j):
        return jnp.bitwise_xor(me, j + 1) if power else lax.rem(me + n - j - 1, n)

    def q_copy(c, slot, peer):
        rows = pl.ds(pl.multiple_of(peer * req_dev + c * part, part), part)
        return send(q_ref.at[rows], qrecv.at[c, slot], q_send.at[c], q_recv_sem.at[c], peer)

    def q_all(c):
        some = qrecv.at[c, pl.ds(0, n - 1)]
        return send(some, some, q_send.at[c], q_recv_sem.at[c], partner)

    def own_copy(slot, peer):
        return send(rp_ref, own_recv.at[slot], own_send, own_recv_sem, peer)

    def own_all():
        some = own_recv.at[pl.ds(0, n - 1)]
        return send(some, some, own_send, own_recv_sem, partner)

    def kv_copy(slot, peer):
        return send(home.at[peer // share], pool.at[slot], kv_send, kv_recv.at[slot], peer)

    def kv_all():
        some = pool.at[pl.ds(0, n // 2 - 1)]
        return send(some, some, kv_send, kv_recv.at[0], partner)

    def fw_copy(slot):
        return send(pool.at[slot], pool.at[slot], fw_send, kv_recv.at[slot], partner)

    def fw_own():
        return send(home.at[me // share], pool.at[me], fw_send, kv_recv.at[me], partner)

    def fw_all():
        some = pool.at[pl.ds(0, n // 2)]
        return send(some, some, fw_send, kv_recv.at[0], partner)

    def ret_copy(c, slot, peer):
        return send(
            retsrc.at[c, peer], retrecv.at[c, slot], ret_send.at[c], ret_recv.at[c, slot], peer
        )

    def ret_all(c):
        some = retsrc.at[c, pl.ds(0, n - 1)]
        return send(some, some, ret_send.at[c], ret_recv.at[c, 0], partner)

    def st_copy(slot, peer):
        return send(stats_src.at[peer], stats_recv.at[slot], st_send, st_recv, peer)

    def st_all():
        some = stats_recv.at[pl.ds(0, n - 1)]
        return send(some, some, st_send, st_recv, partner)

    def q_plane(p, first, last):
        for c in range(CHUNKS):

            @pl.loop(first, last)
            def _(i, c=c):
                q_copy(c, me, p * side + jnp.bitwise_xor(spot, i)).start()

    q_in.wait()
    neighbours = has_up.astype(jnp.int32) + has_down.astype(jnp.int32)
    pl.semaphore_wait(barrier, side - 1 + neighbours)

    @pl.when(has_up)
    def _():
        signal(from_below.at[1], up)
        q_plane(plane + 1, 0, 1)

    @pl.when(has_down)
    def _():
        signal(from_above.at[1], down)
        q_plane(plane - 1, 0, 1)

    q_plane(plane, 1, side)

    @pl.loop(1, planes)
    def _(t):
        above, below = plane + t < planes, plane >= t
        first = jnp.where(t == 1, 1, 0)

        @pl.when(above)
        def _():
            pl.semaphore_wait(from_above.at[t], 1)

            @pl.when(has_down)
            def _():
                signal(from_above.at[t + 1], down)

        @pl.when(below)
        def _():
            pl.semaphore_wait(from_below.at[t], 1)

            @pl.when(has_up)
            def _():
                signal(from_below.at[t + 1], up)

        @pl.when(above)
        def _():
            q_plane(plane + t, first, side)

        @pl.when(below)
        def _():
            q_plane(plane - t, first, side)

    @pl.loop(0, n - 1)
    def _(j):
        own_copy(me, peer_of(j)).start()

    for c in range(CHUNKS):
        qrecv[c, me] = q_ref[pl.ds(pl.multiple_of(me * req_dev + c * part, part), part)]
    own_recv[me] = rp_ref[...]

    kv_in.wait()
    entries = kv_heads * page_len
    entry, source = iota((entries, entries), 0), iota((entries, entries), 1)
    turn = jnp.where(
        source == mod(entry, page_len) * kv_heads + div(entry, page_len), 1.0, 0.0
    ).astype(jnp.bfloat16)
    turned = jnp.dot(turn, kv_ref[...], preferred_element_type=jnp.float32)
    home[...] = turned.astype(jnp.bfloat16).reshape(home.shape)
    pool[me] = home[me // share]

    @pl.loop(1, n // 2)
    def _(j):
        kv_copy(me, lax.rem(me + 2 * j, n)).start()

    fw_own().start()

    size = part * n
    row_id, col_id = iota((size, size), 0), iota((size, size), 1)
    order[...] = jnp.where(
        col_id == mod(row_id, n) * part + div(row_id, n), 1.0, 0.0
    ).astype(jnp.bfloat16)
    back[...] = jnp.where(
        col_id == mod(row_id, part) * n + div(row_id, part), 1.0, 0.0
    ).astype(jnp.bfloat16)
    stacked = iota((per_dev * n, cols), 0)
    head_of_row = mod(stacked, n) * per_dev + div(stacked, n)
    column = iota((per_dev * n, cols), 1)
    own_kv = div(head_of_row, group_size) == mod(column, kv_heads)
    position = jnp.where(own_kv, div(column, kv_heads), cols)
    lane = iota((n, LANES), 1)

    seen = jnp.zeros((n, LANES), jnp.float32)

    @pl.loop(0, req_dev)
    def _(r):
        suf_copy(r).wait()

    for c in range(CHUNKS):
        q_all(c).wait_recv()
        qperm[...] = jnp.dot(
            order[...], qrecv[c].reshape(size, width), preferred_element_type=jnp.float32
        ).astype(jnp.bfloat16)

        def some_requests(step, seen, c=c):
            ids = [step * UNROLL + u for u in range(UNROLL)]
            all_scores = []
            for local in ids:
                r = c * part + local
                rows = pl.ds(pl.multiple_of(local * n, n), n)
                qr = jnp.concatenate(
                    [qperm[rows, h * head_dim:(h + 1) * head_dim] for h in range(per_dev)], axis=0
                )
                all_scores.append(lax.dot_general(
                    qr, suf[r, :, :head_dim], (((1,), (1,)), ((), ())),
                    preferred_element_type=jnp.float32,
                ))
            for local, scores in zip(ids, all_scores):
                r = c * part + local
                rows = pl.ds(pl.multiple_of(local * n, n), n)
                scores = jnp.where(position < len_ref[r], scores, neg_large)
                top_score = jnp.max(scores, axis=1, keepdims=True)
                weight = jnp.exp2((scores - top_score) * scale)
                weight_sum = jnp.sum(weight, axis=1, keepdims=True)
                mixed = jnp.dot(
                    weight.astype(jnp.bfloat16), suf[r, :, head_dim:],
                    preferred_element_type=jnp.float32,
                )
                result = (mixed * (1.0 / weight_sum)).astype(jnp.bfloat16)
                level = top_score * scale + jnp.log(weight_sum) * LOG2E
                for h in range(per_dev):
                    operm[rows, h * head_dim:(h + 1) * head_dim] = result[h * n:(h + 1) * n]
                    seen = jnp.where(
                        lane == h * req_dev + r, level[h * n:(h + 1) * n], seen
                    )
            return seen

        seen = lax.fori_loop(0, part // UNROLL, some_requests, seen)
        if c == CHUNKS - 1:
            for p in range(n):
                stats_src[p] = seen[p:p + 1, :]

            @pl.loop(0, n - 1)
            def _(j):
                st_copy(me, peer_of(j)).start()

        returned = jnp.dot(back[...], operm[...], preferred_element_type=jnp.float32)
        retsrc[c] = returned.astype(jnp.bfloat16).reshape(n, part, width)

        @pl.loop(0, n - 1)
        def _(j, c=c):
            ret_copy(c, me, peer_of(j)).start()

        retrecv[c, me] = retsrc[c, me]
        if c == 0:
            own_all().wait_recv()
            eye = iota((req_dev, req_dev), 0) == iota((req_dev, req_dev), 1)
            for s in range(n):
                own_col[s * req_dev:(s + 1) * req_dev] = jnp.sum(
                    jnp.where(eye, own_recv[s].astype(jnp.float32), 0.0), axis=1, keepdims=True
                )
    stats_recv[me] = stats_src[me]

    @pl.loop(1, n // 2)
    def _(j):
        slot = lax.rem(me + 2 * j, n)
        kv_copy(slot, me).wait_recv()
        fw_copy(slot).start()

    @pl.loop(0, n // 2)
    def _(j):
        slot = lax.rem(partner + 2 * j, n)
        fw_copy(slot).wait_recv()

    tokens = n * page_len
    page = div(iota((1, tokens), 1), page_len)
    token_owner = jnp.zeros((1, tokens), jnp.float32)
    end = jnp.int32(0)
    for i in range(pc_ref.shape[0]):
        end = end + pc_ref[i]
        token_owner = token_owner + jnp.where(page >= end, 1.0, 0.0)

    block = max(32, min(rows_all, PREFIX_KI * 1024 // tokens))

    @pl.loop(0, rows_all // block)
    def _(b):
        rows = pl.ds(pl.multiple_of(b * block, block), block)
        live = own_col[rows] == token_owner
        keys = pool[:, :, :head_dim].reshape(tokens, head_dim)
        values = pool[:, :, head_dim:].reshape(tokens, head_dim)
        for h in range(per_dev):
            scores = lax.dot_general(
                q_ref[rows, h * head_dim:(h + 1) * head_dim], keys, (((1,), (1,)), ((), ())),
                preferred_element_type=jnp.float32,
            )
            scores = jnp.where(live, scores, neg_large)
            top_score = jnp.max(scores, axis=1, keepdims=True)
            weight = jnp.exp2((scores - top_score) * scale)
            top[h, rows] = top_score * scale
            total[h, rows] = jnp.sum(weight, axis=1, keepdims=True)
            mix[rows, h * head_dim:(h + 1) * head_dim] = jnp.dot(
                weight.astype(jnp.bfloat16), values, preferred_element_type=jnp.float32
            )

    for c in range(CHUNKS):
        q_all(c).wait_send()
    own_all().wait_send()
    kv_all().wait_send()
    fw_all().wait_send()

    st_all().wait_recv()
    sub, lan = iota((req_dev, LANES), 0), iota((req_dev, LANES), 1)

    @pl.loop(0, n // 2)
    def _(step):
        for u in range(2):
            s = step * 2 + u
            rows = pl.ds(pl.multiple_of(s * req_dev, req_dev), req_dev)
            row = stats_recv[s]
            for h in range(per_dev):
                span = slice(h * head_dim, (h + 1) * head_dim)
                level = jnp.sum(
                    jnp.where(lan == h * req_dev + sub, row, 0.0), axis=1, keepdims=True
                )
                top_first = top[h, rows]
                top_score = jnp.maximum(level, top_first)
                factor_second = jnp.exp2(level - top_score)
                factor_first = jnp.exp2(top_first - top_score)
                inverse = 1.0 / (total[h, rows] * factor_first + factor_second)
                mix[rows, span] = mix[rows, span] * (factor_first * inverse)
                second_factor[rows, span] = jnp.broadcast_to(
                    factor_second * inverse, (req_dev, head_dim)
                )

    def gather_in(c, s):
        rows = pl.ds(pl.multiple_of(s * req_dev + c * part, part), part)
        second = retrecv[c, s].astype(jnp.float32)
        out_ref[rows, :] = (mix[rows, :] + second * second_factor[rows, :]).astype(out_ref.dtype)

    for c in range(CHUNKS):
        gather_in(c, me)

        @pl.loop(0, n - 1)
        def _(j, c=c):
            slot = source_of(j)
            ret_copy(c, slot, me).wait_recv()
            gather_in(c, slot)

    st_all().wait_send()
    for c in range(CHUNKS):
        ret_all(c).wait_send()


def body(queries, prefix_kv, page_counts, request_prefix, suffix_kv, suffix_len):
    n = lax.axis_size("blk")
    rows_all, width = queries.shape
    req_dev, suf_len, kv_heads, kv_width = suffix_kv.shape
    head_dim = kv_width // 2
    per_dev = width // head_dim
    page_len = prefix_kv.shape[1]
    part = req_dev // CHUNKS
    page = prefix_kv.reshape(page_len * kv_heads, kv_width)
    cache = suffix_kv.reshape(req_dev, suf_len * kv_heads, kv_width)
    bf16, f32, i32 = jnp.bfloat16, jnp.float32, jnp.int32
    dma, regular = pltpu.SemaphoreType.DMA, pltpu.SemaphoreType.REGULAR
    vmem = pl.BlockSpec(memory_space=pltpu.VMEM)
    smem = pl.BlockSpec(memory_space=pltpu.SMEM)
    anywhere = pl.BlockSpec(memory_space=pl.ANY)
    return pl.pallas_call(
        functools.partial(kernel, n),
        out_shape=pltpu.VMEM((rows_all, width), bf16),
        in_specs=[anywhere, anywhere, vmem, smem, anywhere, smem],
        out_specs=vmem,
        scratch_shapes=[
            pltpu.VMEM((rows_all, width), bf16),
            pltpu.VMEM((page_len * kv_heads, kv_width), bf16),
            pltpu.VMEM((kv_heads, page_len, kv_width), bf16),
            pltpu.VMEM((part * n, part * n), bf16),
            pltpu.VMEM((part * n, part * n), bf16),
            pltpu.VMEM((CHUNKS, n, part, width), bf16),
            pltpu.VMEM((part * n, width), bf16),
            pltpu.VMEM((part * n, width), bf16),
            pltpu.VMEM((CHUNKS, n, part, width), bf16),
            pltpu.VMEM((CHUNKS, n, part, width), bf16),
            pltpu.VMEM((n, page_len, kv_width), bf16),
            pltpu.VMEM((req_dev, suf_len * kv_heads, kv_width), bf16),
            pltpu.VMEM((n, 1, req_dev), i32),
            pltpu.VMEM((rows_all, 1), f32),
            pltpu.VMEM((n, 1, LANES), f32),
            pltpu.VMEM((n, 1, LANES), f32),
            pltpu.VMEM((rows_all, width), f32),
            pltpu.VMEM((rows_all, width), f32),
            pltpu.VMEM((per_dev, rows_all, 1), f32),
            pltpu.VMEM((per_dev, rows_all, 1), f32),
            dma((CHUNKS,)), dma((CHUNKS,)), dma, dma, dma, dma((n,)), dma,
            dma((CHUNKS,)), dma((CHUNKS, n)), dma, dma, dma((req_dev,)), dma((2,)),
            regular((n // plane_of(n) + 1,)), regular((n // plane_of(n) + 1,)),
        ],
        compiler_params=pltpu.CompilerParams(
            collective_id=0, has_side_effects=True, vmem_limit_bytes=VMEM_MIB * 1024 * 1024
        ),
    )(queries, page, request_prefix.T, page_counts, cache, suffix_len)


def solution(mesh):
    in_specs = (
        P("groups", "blk"),
        P(("groups", "blk"), None, None, None),
        P("groups"),
        P(("groups", "blk"), None),
        P(("groups", "blk"), None, None, None),
        P(("groups", "blk")),
    )
    out_specs = P("groups", "blk")
    return jax.shard_map(body, mesh=mesh, in_specs=in_specs, out_specs=out_specs, check_vma=False)
```

```python
import functools
import math

import jax
import jax.numpy as jnp
from jax import lax
from jax.experimental import pallas as pl
from jax.experimental.pallas import tpu as pltpu
from jax.sharding import PartitionSpec as P

neg_large = -1e30


def div(x, k):
    return jnp.right_shift(x, k.bit_length() - 1) if k & (k - 1) == 0 else x // k


def mod(x, k):
    return jnp.bitwise_and(x, k - 1) if k & (k - 1) == 0 else lax.rem(x, k)


MESH = pl.DeviceIdType.MESH
CHUNKS = 2
UNROLL = 8
LANES = 128
PREFIX_KI = 256
VMEM_MIB = 56
LOG2E = math.log2(math.e)


def plane_of(n):
    bits = n.bit_length() - 1
    return 1 << (bits + 1) // 2 if n & (n - 1) == 0 else 1


def kernel(
    n, q_hbm, kv_hbm, rp_hbm, pc_hbm, suf_ref, len_hbm, out_ref,
    rp_ref, pc_ref, len_ref, q_ref, kv_ref, home, order, back, qrecv, qperm, operm, retsrc, retrecv, pool, suf, own_recv,
    own_col, stats_src, stats_recv, mix, second_factor, top, total,
    q_send, q_recv_sem, own_send, own_recv_sem, kv_send, kv_recv, fw_send,
    ret_send, ret_recv, st_send, st_recv, suf_sem, in_sem, from_below, from_above,
):
    me = lax.axis_index("blk")
    partner = me + 1 - 2 * lax.rem(me, 2)
    rows_all, width = q_ref.shape
    req_dev = rows_all // n
    part = req_dev // CHUNKS
    kv_heads, page_len, kv_width = home.shape
    head_dim = kv_width // 2
    per_dev = width // head_dim
    heads = per_dev * n
    group_size = heads // kv_heads
    share = n // kv_heads
    cols = suf_ref.shape[1]
    scale = head_dim ** -0.5 * LOG2E
    power = n & (n - 1) == 0

    def iota(shape, dim):
        return lax.broadcasted_iota(jnp.int32, shape, dim)

    def signal(sem, peer):
        pl.semaphore_signal(sem, inc=1, device_id={"blk": peer}, device_id_type=MESH)

    barrier = pltpu.get_barrier_semaphore()
    side = plane_of(n)
    planes = n // side
    plane, spot = div(me, side), mod(me, side)
    has_up, has_down = plane + 1 < planes, plane > 0
    up, down = lax.rem(me + side, n), lax.rem(me + n - side, n)

    @pl.loop(0, side)
    def _(k):
        spot_k = jnp.bitwise_xor(spot, k)

        @pl.when(has_up)
        def _():
            signal(barrier, (plane + 1) * side + spot_k)

        @pl.when(has_down)
        def _():
            signal(barrier, (plane - 1) * side + spot_k)

        @pl.when(k > 0)
        def _():
            signal(barrier, plane * side + spot_k)

    q_in = pltpu.make_async_copy(q_hbm, q_ref, in_sem.at[0])
    kv_in = pltpu.make_async_copy(kv_hbm, kv_ref, in_sem.at[1])
    small_in = [
        pltpu.make_async_copy(src, dst, in_sem.at[2 + i])
        for i, (src, dst) in enumerate(((rp_hbm, rp_ref), (pc_hbm, pc_ref), (len_hbm, len_ref)))
    ]
    q_in.start()
    kv_in.start()
    for copy in small_in:
        copy.start()

    def suf_copy(r):
        return pltpu.make_async_copy(suf_ref.at[r], suf.at[r], suf_sem.at[r])

    @pl.loop(0, req_dev)
    def _(r):
        suf_copy(r).start()

    def send(src, dst, s_sem, r_sem, peer):
        return pltpu.make_async_remote_copy(
            src_ref=src, dst_ref=dst, send_sem=s_sem, recv_sem=r_sem,
            device_id={"blk": peer}, device_id_type=MESH,
        )

    half = n // 2 if planes % 2 == 0 else n
    base = div(me, half) * half
    lower = me < half

    def peer_of(j):
        return jnp.bitwise_xor(me, j + 1) if power else lax.rem(me + j + 1, n)

    def local_of(j):
        return jnp.bitwise_xor(me, j + 1) if power else base + lax.rem(me - base + j + 1, half)

    def across_of(t, i):
        p = jnp.where(lower, planes - 1 - t, t)
        return p * side + jnp.bitwise_xor(spot, i)

    def q_copy(c, slot, peer):
        rows = pl.ds(pl.multiple_of(peer * req_dev + c * part, part), part)
        return send(q_ref.at[rows], qrecv.at[c, slot], q_send.at[c], q_recv_sem.at[c], peer)

    def q_all(c):
        some = qrecv.at[c, pl.ds(0, n - 1)]
        return send(some, some, q_send.at[c], q_recv_sem.at[c], partner)

    def own_copy(slot, peer):
        return send(rp_ref, own_recv.at[slot], own_send, own_recv_sem, peer)

    def own_all():
        some = own_recv.at[pl.ds(0, n - 1)]
        return send(some, some, own_send, own_recv_sem, partner)

    def kv_copy(slot, peer):
        return send(home.at[peer // share], pool.at[slot], kv_send, kv_recv.at[slot], peer)

    def kv_all():
        some = pool.at[pl.ds(0, n // 2 - 1)]
        return send(some, some, kv_send, kv_recv.at[0], partner)

    def fw_copy(slot):
        return send(pool.at[slot], pool.at[slot], fw_send, kv_recv.at[slot], partner)

    def fw_own():
        return send(home.at[me // share], pool.at[me], fw_send, kv_recv.at[me], partner)

    def fw_all():
        some = pool.at[pl.ds(0, n // 2)]
        return send(some, some, fw_send, kv_recv.at[0], partner)

    def ret_copy(c, slot, peer):
        return send(
            retsrc.at[c, peer], retrecv.at[c, slot], ret_send.at[c], ret_recv.at[c, slot], peer
        )

    def ret_across(c, first, last):
        @pl.loop(first * side, last * side)
        def _(j):
            ret_copy(c, me, across_of(div(j, side), mod(j, side))).start()

    def ret_all(c):
        some = retsrc.at[c, pl.ds(0, n - 1)]
        return send(some, some, ret_send.at[c], ret_recv.at[c, 0], partner)

    def st_copy(slot, peer):
        return send(stats_src.at[peer], stats_recv.at[slot], st_send, st_recv, peer)

    def st_all():
        some = stats_recv.at[pl.ds(0, n - 1)]
        return send(some, some, st_send, st_recv, partner)

    def q_plane(p, first, last, chunks):
        for c in chunks:

            @pl.loop(first, last)
            def _(i, c=c):
                q_copy(c, me, p * side + jnp.bitwise_xor(spot, i)).start()

    neighbours = has_up.astype(jnp.int32) + has_down.astype(jnp.int32)
    pl.semaphore_wait(barrier, side - 1 + side * neighbours)

    @pl.when(has_up & has_down)
    def _():
        signal(from_below.at[2], up)
        signal(from_above.at[2], down)

    q_in.wait()

    def near(chunks):
        @pl.when(has_up)
        def _():
            q_plane(plane + 1, 0, side, chunks)

        @pl.when(has_down)
        def _():
            q_plane(plane - 1, 0, side, chunks)

        q_plane(plane, 1, side, chunks)

    def far(c, relay):
        @pl.loop(2, planes)
        def _(t):
            above, below = plane + t < planes, plane >= t
            if relay:

                @pl.when(above)
                def _():
                    pl.semaphore_wait(from_above.at[t], 1)

                    @pl.when(has_down)
                    def _():
                        signal(from_above.at[t + 1], down)

                @pl.when(below)
                def _():
                    pl.semaphore_wait(from_below.at[t], 1)

                    @pl.when(has_up)
                    def _():
                        signal(from_below.at[t + 1], up)

            @pl.when(above)
            def _():
                q_plane(plane + t, 0, side, (c,))

            @pl.when(below)
            def _():
                q_plane(plane - t, 0, side, (c,))

    def send_own():
        for copy in small_in:
            copy.wait()

        @pl.loop(0, n - 1)
        def _(j):
            own_copy(me, peer_of(j)).start()

        own_recv[me] = rp_ref[...]

    def keep_mine():
        for c in range(CHUNKS):
            qrecv[c, me] = q_ref[pl.ds(pl.multiple_of(me * req_dev + c * part, part), part)]

    def turn_page():
        kv_in.wait()
        entries = kv_heads * page_len
        entry, source = iota((entries, entries), 0), iota((entries, entries), 1)
        turn = jnp.where(
            source == mod(entry, page_len) * kv_heads + div(entry, page_len), 1.0, 0.0
        ).astype(jnp.bfloat16)
        turned = jnp.dot(turn, kv_ref[...], preferred_element_type=jnp.float32)
        home[...] = turned.astype(jnp.bfloat16).reshape(home.shape)
        pool[me] = home[me // share]

    def send_pages():
        @pl.loop(1, n // 2)
        def _(j):
            kv_copy(me, lax.rem(me + 2 * j, n)).start()

        fw_own().start()

    size = part * n

    def make_orders():
        row_id, col_id = iota((size, size), 0), iota((size, size), 1)
        order[...] = jnp.where(
            col_id == mod(row_id, n) * part + div(row_id, n), 1.0, 0.0
        ).astype(jnp.bfloat16)
        back[...] = jnp.where(
            col_id == mod(row_id, part) * n + div(row_id, part), 1.0, 0.0
        ).astype(jnp.bfloat16)

    def suffix_in():
        @pl.loop(0, req_dev)
        def _(r):
            suf_copy(r).wait()

    def suffix(c, seen):
        stacked = iota((per_dev * n, cols), 0)
        head_of_row = mod(stacked, n) * per_dev + div(stacked, n)
        column = iota((per_dev * n, cols), 1)
        own_kv = div(head_of_row, group_size) == mod(column, kv_heads)
        position = jnp.where(own_kv, div(column, kv_heads), cols)
        lane = iota((n, LANES), 1)
        qperm[...] = jnp.dot(
            order[...], qrecv[c].reshape(size, width), preferred_element_type=jnp.float32
        ).astype(jnp.bfloat16)

        def some_requests(step, seen):
            ids = [step * UNROLL + u for u in range(UNROLL)]
            all_scores = []
            for local in ids:
                rows = pl.ds(pl.multiple_of(local * n, n), n)
                qr = jnp.concatenate(
                    [qperm[rows, h * head_dim:(h + 1) * head_dim] for h in range(per_dev)], axis=0
                )
                all_scores.append(lax.dot_general(
                    qr, suf[c * part + local, :, :head_dim], (((1,), (1,)), ((), ())),
                    preferred_element_type=jnp.float32,
                ))
            for local, scores in zip(ids, all_scores):
                r = c * part + local
                rows = pl.ds(pl.multiple_of(local * n, n), n)
                scores = jnp.where(position < len_ref[r], scores, neg_large)
                top_score = jnp.max(scores, axis=1, keepdims=True)
                weight = jnp.exp2((scores - top_score) * scale)
                weight_sum = jnp.sum(weight, axis=1, keepdims=True)
                mixed = jnp.dot(
                    weight.astype(jnp.bfloat16), suf[r, :, head_dim:],
                    preferred_element_type=jnp.float32,
                )
                result = (mixed * (1.0 / weight_sum)).astype(jnp.bfloat16)
                level = top_score * scale + jnp.log(weight_sum) * LOG2E
                for h in range(per_dev):
                    operm[rows, h * head_dim:(h + 1) * head_dim] = result[h * n:(h + 1) * n]
                    seen = jnp.where(
                        lane == h * req_dev + r, level[h * n:(h + 1) * n], seen
                    )
            return seen

        seen = lax.fori_loop(0, part // UNROLL, some_requests, seen)
        returned = jnp.dot(back[...], operm[...], preferred_element_type=jnp.float32)
        retsrc[c] = returned.astype(jnp.bfloat16).reshape(n, part, width)
        retrecv[c, me] = retsrc[c, me]
        return seen

    def send_stats(seen):
        for p in range(n):
            stats_src[p] = seen[p:p + 1, :]

        @pl.loop(0, n - 1)
        def _(j):
            st_copy(me, peer_of(j)).start()

        stats_recv[me] = stats_src[me]

    def send_back_near(c):
        @pl.loop(0, half - 1)
        def _(j):
            ret_copy(c, me, local_of(j)).start()

    def send_back_across(c):
        if half < n:
            ret_across(c, 0, planes // 2)

    def take_own():
        own_all().wait_recv()
        eye = iota((req_dev, req_dev), 0) == iota((req_dev, req_dev), 1)
        for s in range(n):
            own_col[s * req_dev:(s + 1) * req_dev] = jnp.sum(
                jnp.where(eye, own_recv[s].astype(jnp.float32), 0.0), axis=1, keepdims=True
            )

    def pass_pages():
        @pl.loop(1, n // 2)
        def _(j):
            slot = lax.rem(me + 2 * j, n)
            kv_copy(slot, me).wait_recv()
            fw_copy(slot).start()

    def take_pages():
        @pl.loop(0, n // 2)
        def _(j):
            slot = lax.rem(partner + 2 * j, n)
            fw_copy(slot).wait_recv()

    def prefix():
        tokens = n * page_len
        page = div(iota((1, tokens), 1), page_len)
        token_owner = jnp.zeros((1, tokens), jnp.float32)
        end = jnp.int32(0)
        for i in range(pc_ref.shape[0]):
            end = end + pc_ref[i]
            token_owner = token_owner + jnp.where(page >= end, 1.0, 0.0)

        block = max(32, min(rows_all, PREFIX_KI * 1024 // tokens))

        @pl.loop(0, rows_all // block)
        def _(b):
            rows = pl.ds(pl.multiple_of(b * block, block), block)
            live = own_col[rows] == token_owner
            keys = pool[:, :, :head_dim].reshape(tokens, head_dim)
            values = pool[:, :, head_dim:].reshape(tokens, head_dim)
            for h in range(per_dev):
                span = slice(h * head_dim, (h + 1) * head_dim)
                scores = lax.dot_general(
                    q_ref[rows, span], keys, (((1,), (1,)), ((), ())),
                    preferred_element_type=jnp.float32,
                )
                scores = jnp.where(live, scores, neg_large)
                top_score = jnp.max(scores, axis=1, keepdims=True)
                weight = jnp.exp2((scores - top_score) * scale)
                top[h, rows] = top_score * scale
                total[h, rows] = jnp.sum(weight, axis=1, keepdims=True)
                mix[rows, span] = jnp.dot(
                    weight.astype(jnp.bfloat16), values, preferred_element_type=jnp.float32
                )

    def factors():
        st_all().wait_recv()
        sub, lan = iota((req_dev, LANES), 0), iota((req_dev, LANES), 1)

        @pl.loop(0, n // 2)
        def _(step):
            for u in range(2):
                s = step * 2 + u
                rows = pl.ds(pl.multiple_of(s * req_dev, req_dev), req_dev)
                row = stats_recv[s]
                for h in range(per_dev):
                    span = slice(h * head_dim, (h + 1) * head_dim)
                    level = jnp.sum(
                        jnp.where(lan == h * req_dev + sub, row, 0.0), axis=1, keepdims=True
                    )
                    top_first = top[h, rows]
                    top_score = jnp.maximum(level, top_first)
                    factor_second = jnp.exp2(level - top_score)
                    factor_first = jnp.exp2(top_first - top_score)
                    inverse = 1.0 / (total[h, rows] * factor_first + factor_second)
                    mix[rows, span] = mix[rows, span] * (factor_first * inverse)
                    second_factor[rows, span] = jnp.broadcast_to(
                        factor_second * inverse, (req_dev, head_dim)
                    )

    def gather_in(c, s):
        rows = pl.ds(pl.multiple_of(s * req_dev + c * part, part), part)
        second = retrecv[c, s].astype(jnp.float32)
        out_ref[rows, :] = (mix[rows, :] + second * second_factor[rows, :]).astype(out_ref.dtype)

    def arrive(c, slot):
        ret_copy(c, slot, me).wait_recv()
        gather_in(c, slot)

    def gather_near(c):
        gather_in(c, me)

        @pl.loop(0, half - 1)
        def _(j):
            arrive(c, local_of(j))

    def gather_across(c):
        if half < n:

            @pl.loop(0, half)
            def _(j):
                arrive(c, across_of(div(j, side), mod(j, side)))

    seen = jnp.zeros((n, LANES), jnp.float32)
    near((0, 1))
    far(0, True)
    far(1, False)
    send_own()
    keep_mine()
    turn_page()
    send_pages()
    make_orders()
    suffix_in()
    q_all(0).wait_recv()
    seen = suffix(0, seen)
    send_back_near(0)
    send_back_across(0)
    take_own()
    q_all(1).wait_recv()
    seen = suffix(1, seen)
    send_stats(seen)
    send_back_near(1)
    send_back_across(1)
    pass_pages()
    take_pages()
    prefix()
    q_all(0).wait_send()
    q_all(1).wait_send()
    own_all().wait_send()
    kv_all().wait_send()
    fw_all().wait_send()
    factors()
    gather_near(0)
    gather_near(1)
    gather_across(0)
    gather_across(1)
    st_all().wait_send()
    ret_all(0).wait_send()
    ret_all(1).wait_send()


def body(queries, prefix_kv, page_counts, request_prefix, suffix_kv, suffix_len):
    n = lax.axis_size("blk")
    rows_all, width = queries.shape
    req_dev, suf_len, kv_heads, kv_width = suffix_kv.shape
    head_dim = kv_width // 2
    per_dev = width // head_dim
    page_len = prefix_kv.shape[1]
    part = req_dev // CHUNKS
    page = prefix_kv.reshape(page_len * kv_heads, kv_width)
    cache = suffix_kv.reshape(req_dev, suf_len * kv_heads, kv_width)
    bf16, f32, i32 = jnp.bfloat16, jnp.float32, jnp.int32
    dma, regular = pltpu.SemaphoreType.DMA, pltpu.SemaphoreType.REGULAR
    vmem = pl.BlockSpec(memory_space=pltpu.VMEM)
    anywhere = pl.BlockSpec(memory_space=pl.ANY)
    return pl.pallas_call(
        functools.partial(kernel, n),
        out_shape=pltpu.VMEM((rows_all, width), bf16),
        in_specs=[anywhere] * 6,
        out_specs=vmem,
        scratch_shapes=[
            pltpu.VMEM((1, req_dev), i32),
            pltpu.SMEM(page_counts.shape, i32),
            pltpu.SMEM((req_dev,), i32),
            pltpu.VMEM((rows_all, width), bf16),
            pltpu.VMEM((page_len * kv_heads, kv_width), bf16),
            pltpu.VMEM((kv_heads, page_len, kv_width), bf16),
            pltpu.VMEM((part * n, part * n), bf16),
            pltpu.VMEM((part * n, part * n), bf16),
            pltpu.VMEM((CHUNKS, n, part, width), bf16),
            pltpu.VMEM((part * n, width), bf16),
            pltpu.VMEM((part * n, width), bf16),
            pltpu.VMEM((CHUNKS, n, part, width), bf16),
            pltpu.VMEM((CHUNKS, n, part, width), bf16),
            pltpu.VMEM((n, page_len, kv_width), bf16),
            pltpu.VMEM((req_dev, suf_len * kv_heads, kv_width), bf16),
            pltpu.VMEM((n, 1, req_dev), i32),
            pltpu.VMEM((rows_all, 1), f32),
            pltpu.VMEM((n, 1, LANES), f32),
            pltpu.VMEM((n, 1, LANES), f32),
            pltpu.VMEM((rows_all, width), f32),
            pltpu.VMEM((rows_all, width), f32),
            pltpu.VMEM((per_dev, rows_all, 1), f32),
            pltpu.VMEM((per_dev, rows_all, 1), f32),
            dma((CHUNKS,)), dma((CHUNKS,)), dma, dma, dma, dma((n,)), dma,
            dma((CHUNKS,)), dma((CHUNKS, n)), dma, dma, dma((req_dev,)), dma((5,)),
            regular((n // plane_of(n) + 1,)), regular((n // plane_of(n) + 1,)),
        ],
        compiler_params=pltpu.CompilerParams(
            collective_id=0, has_side_effects=True, vmem_limit_bytes=VMEM_MIB * 1024 * 1024
        ),
    )(queries, page, request_prefix.T, page_counts, cache, suffix_len)


def solution(mesh):
    in_specs = (
        P("groups", "blk"),
        P(("groups", "blk"), None, None, None),
        P("groups"),
        P(("groups", "blk"), None),
        P(("groups", "blk"), None, None, None),
        P(("groups", "blk")),
    )
    out_specs = P("groups", "blk")
    return jax.shard_map(body, mesh=mesh, in_specs=in_specs, out_specs=out_specs, check_vma=False)
```

```python
import functools
import math

import jax
import jax.numpy as jnp
from jax import lax
from jax.experimental import pallas as pl
from jax.experimental.pallas import tpu as pltpu
from jax.sharding import PartitionSpec as P

neg_large = -1e30


def div(x, k):
    return jnp.right_shift(x, k.bit_length() - 1) if k & (k - 1) == 0 else x // k


def mod(x, k):
    return jnp.bitwise_and(x, k - 1) if k & (k - 1) == 0 else lax.rem(x, k)


MESH = pl.DeviceIdType.MESH
CHUNKS = 2
UNROLL = 8
NEAR = 1
LANES = 128
PREFIX_KI = 256
VMEM_MIB = 56
LOG2E = math.log2(math.e)


def plane_of(n):
    bits = n.bit_length() - 1
    return 1 << (bits + 1) // 2 if n & (n - 1) == 0 else 1


def kernel(
    n, q_hbm, kv_hbm, rp_hbm, pc_hbm, suf_ref, len_hbm, out_ref,
    rp_ref, pc_ref, len_ref, q_ref, kv_ref, home, order, back, qrecv, qperm, operm, retsrc, retrecv, pool, suf, own_recv,
    own_col, stats_src, stats_recv, mix, second_factor, top, total,
    q_send, q_recv_sem, own_send, own_recv_sem, kv_send, kv_recv, fw_send, fw_recv,
    ret_send, ret_recv, st_send, st_recv, suf_sem, in_sem, reply,
):
    me = lax.axis_index("blk")
    partner = me + 1 - 2 * lax.rem(me, 2)
    rows_all, width = q_ref.shape
    req_dev = rows_all // n
    part = req_dev // CHUNKS
    kv_heads, page_len, kv_width = home.shape
    head_dim = kv_width // 2
    per_dev = width // head_dim
    heads = per_dev * n
    group_size = heads // kv_heads
    share = n // kv_heads
    cols = suf_ref.shape[1]
    scale = head_dim ** -0.5 * LOG2E
    power = n & (n - 1) == 0

    def iota(shape, dim):
        return lax.broadcasted_iota(jnp.int32, shape, dim)

    def signal(sem, peer):
        pl.semaphore_signal(sem, inc=1, device_id={"blk": peer}, device_id_type=MESH)

    barrier = pltpu.get_barrier_semaphore()
    side = plane_of(n)
    planes = n // side
    plane, spot = div(me, side), mod(me, side)

    @pl.loop(me + 1, n)
    def _(p):
        signal(barrier, p)

    q_in = pltpu.make_async_copy(q_hbm, q_ref, in_sem.at[0])
    kv_in = pltpu.make_async_copy(kv_hbm, kv_ref, in_sem.at[1])
    small_in = [
        pltpu.make_async_copy(src, dst, in_sem.at[2 + i])
        for i, (src, dst) in enumerate(((rp_hbm, rp_ref), (pc_hbm, pc_ref), (len_hbm, len_ref)))
    ]
    q_in.start()
    kv_in.start()
    for copy in small_in:
        copy.start()

    def suf_copy(r):
        return pltpu.make_async_copy(suf_ref.at[r], suf.at[r], suf_sem)

    @pl.loop(0, req_dev)
    def _(r):
        suf_copy(r).start()

    def send(src, dst, s_sem, r_sem, peer):
        return pltpu.make_async_remote_copy(
            src_ref=src, dst_ref=dst, send_sem=s_sem, recv_sem=r_sem,
            device_id={"blk": peer}, device_id_type=MESH,
        )

    half = n // 2 if planes % 2 == 0 else n
    base = div(me, half) * half
    lower = me < half
    middle = (plane == planes // 2) | (plane == planes // 2 - 1)

    def peer_of(j):
        return jnp.bitwise_xor(me, j + 1) if power else lax.rem(me + j + 1, n)

    def local_of(j):
        return jnp.bitwise_xor(me, j + 1) if power else base + lax.rem(me - base + j + 1, half)

    def across_of(t, i):
        p = jnp.where(lower, planes - 1 - t, t)
        return p * side + jnp.bitwise_xor(spot, i)

    def q_copy(c, slot, peer):
        rows = pl.ds(pl.multiple_of(peer * req_dev + c * part, part), part)
        return send(q_ref.at[rows], qrecv.at[c, slot], q_send.at[c], q_recv_sem.at[c], peer)

    def q_all(c):
        some = qrecv.at[c, pl.ds(0, n - 1)]
        return send(some, some, q_send.at[c], q_recv_sem.at[c], partner)

    def own_copy(slot, peer):
        return send(rp_ref, own_recv.at[slot], own_send, own_recv_sem, peer)

    def own_all():
        some = own_recv.at[pl.ds(0, n - 1)]
        return send(some, some, own_send, own_recv_sem, partner)

    def kv_copy(slot, peer):
        return send(home.at[peer // share], pool.at[slot], kv_send, kv_recv, peer)

    def kv_all():
        some = pool.at[pl.ds(0, n // 2 - 1)]
        return send(some, some, kv_send, kv_recv, partner)

    def fw_copy(slot):
        return send(pool.at[slot], pool.at[slot], fw_send, fw_recv, partner)

    def fw_own():
        return send(home.at[me // share], pool.at[me], fw_send, fw_recv, partner)

    def fw_all():
        some = pool.at[pl.ds(0, n // 2)]
        return send(some, some, fw_send, fw_recv, partner)

    def ret_copy(c, slot, peer, group):
        return send(
            retsrc.at[c, peer], retrecv.at[c, slot], ret_send.at[c], ret_recv.at[c, group], peer
        )

    def ret_across(c, first, last):
        @pl.loop(first * side, last * side)
        def _(j):
            ret_copy(c, me, across_of(div(j, side), mod(j, side)), 1).start()

    def ret_all(c):
        some = retsrc.at[c, pl.ds(0, n - 1)]
        return send(some, some, ret_send.at[c], ret_recv.at[c, 0], partner)

    def st_copy(slot, peer):
        return send(stats_src.at[peer], stats_recv.at[slot], st_send, st_recv, peer)

    def st_all():
        some = stats_recv.at[pl.ds(0, n - 1)]
        return send(some, some, st_send, st_recv, partner)

    @pl.when(me > 0)
    def _():
        pl.semaphore_wait(barrier, me)


    @pl.loop(0, me)
    def _(j):
        signal(reply.at[me], me - 1 - j)

    q_in.wait()
    def home_plane(c, later):
        @pl.loop(1, side)
        def _(i):
            p = plane * side + jnp.bitwise_xor(spot, i)

            @pl.when(p > me if later else p < me)
            def _():
                if later and c == 0:
                    pl.semaphore_wait(reply.at[p], 1)
                q_copy(c, me, p).start()

    def to_plane(c, z, wait):
        @pl.loop(0, side)
        def _(i):
            p = z * side + jnp.bitwise_xor(spot, i)
            if wait:
                pl.semaphore_wait(reply.at[p], 1)
            q_copy(c, me, p).start()

    def to_earlier(c):
        home_plane(c, False)

        @pl.loop(0, plane)
        def _(j):
            to_plane(c, plane - 1 - j, False)

    def to_later():
        home_plane(0, True)
        home_plane(1, True)
        reach = jnp.minimum(plane + NEAR, planes)

        @pl.loop(plane + 1, reach)
        def _(z):
            to_plane(0, z, True)
            to_plane(1, z, False)

        @pl.loop(reach, planes)
        def _(z):
            to_plane(0, z, True)

    def to_last():
        @pl.loop(jnp.minimum(plane + NEAR, planes), planes)
        def _(z):
            to_plane(1, z, False)

    def send_own():
        for copy in small_in:
            copy.wait()

        @pl.loop(0, n - 1)
        def _(j):
            own_copy(me, peer_of(j)).start()

        own_recv[me] = rp_ref[...]

    def keep_mine():
        for c in range(CHUNKS):
            qrecv[c, me] = q_ref[pl.ds(pl.multiple_of(me * req_dev + c * part, part), part)]

    def turn_page():
        kv_in.wait()
        entries = kv_heads * page_len
        entry, source = iota((entries, entries), 0), iota((entries, entries), 1)
        turn = jnp.where(
            source == mod(entry, page_len) * kv_heads + div(entry, page_len), 1.0, 0.0
        ).astype(jnp.bfloat16)
        turned = jnp.dot(turn, kv_ref[...], preferred_element_type=jnp.float32)
        home[...] = turned.astype(jnp.bfloat16).reshape(home.shape)
        pool[me] = home[me // share]

    def send_pages():
        @pl.loop(1, n // 2)
        def _(j):
            kv_copy(me, lax.rem(me + 2 * j, n)).start()

        fw_own().start()

    size = part * n

    def make_orders():
        row_id, col_id = iota((size, size), 0), iota((size, size), 1)
        order[...] = jnp.where(
            col_id == mod(row_id, n) * part + div(row_id, n), 1.0, 0.0
        ).astype(jnp.bfloat16)
        back[...] = jnp.where(
            col_id == mod(row_id, part) * n + div(row_id, part), 1.0, 0.0
        ).astype(jnp.bfloat16)

    def suffix_in():
        pltpu.make_async_copy(suf_ref, suf, suf_sem).wait()

    def suffix(c, seen):
        stacked = iota((per_dev * n, cols), 0)
        head_of_row = mod(stacked, n) * per_dev + div(stacked, n)
        column = iota((per_dev * n, cols), 1)
        own_kv = div(head_of_row, group_size) == mod(column, kv_heads)
        position = jnp.where(own_kv, div(column, kv_heads), cols)
        lane = iota((n, LANES), 1)
        qperm[...] = jnp.dot(
            order[...], qrecv[c].reshape(size, width), preferred_element_type=jnp.float32
        ).astype(jnp.bfloat16)

        def some_requests(step, seen):
            ids = [step * UNROLL + u for u in range(UNROLL)]
            all_scores = []
            for local in ids:
                rows = pl.ds(pl.multiple_of(local * n, n), n)
                qr = jnp.concatenate(
                    [qperm[rows, h * head_dim:(h + 1) * head_dim] for h in range(per_dev)], axis=0
                )
                all_scores.append(lax.dot_general(
                    qr, suf[c * part + local, :, :head_dim], (((1,), (1,)), ((), ())),
                    preferred_element_type=jnp.float32,
                ))
            for local, scores in zip(ids, all_scores):
                r = c * part + local
                rows = pl.ds(pl.multiple_of(local * n, n), n)
                scores = jnp.where(position < len_ref[r], scores, neg_large)
                top_score = jnp.max(scores, axis=1, keepdims=True)
                weight = jnp.exp2((scores - top_score) * scale)
                weight_sum = jnp.sum(weight, axis=1, keepdims=True)
                mixed = jnp.dot(
                    weight.astype(jnp.bfloat16), suf[r, :, head_dim:],
                    preferred_element_type=jnp.float32,
                )
                result = (mixed * (1.0 / weight_sum)).astype(jnp.bfloat16)
                level = top_score * scale + jnp.log(weight_sum) * LOG2E
                for h in range(per_dev):
                    operm[rows, h * head_dim:(h + 1) * head_dim] = result[h * n:(h + 1) * n]
                    seen = jnp.where(
                        lane == h * req_dev + r, level[h * n:(h + 1) * n], seen
                    )
            return seen

        seen = lax.fori_loop(0, part // UNROLL, some_requests, seen)
        returned = jnp.dot(back[...], operm[...], preferred_element_type=jnp.float32)
        retsrc[c] = returned.astype(jnp.bfloat16).reshape(n, part, width)
        retrecv[c, me] = retsrc[c, me]
        return seen

    def send_stats(seen):
        for p in range(n):
            stats_src[p] = seen[p:p + 1, :]

        @pl.loop(0, n - 1)
        def _(j):
            st_copy(me, peer_of(j)).start()

        stats_recv[me] = stats_src[me]

    def send_back_near(c):
        @pl.loop(0, half - 1)
        def _(j):
            ret_copy(c, me, local_of(j), 0).start()

    def send_back_across(c, part=0):
        if half < n:
            if part == 0:
                ret_across(c, 0, planes // 2 - 1)

                @pl.when(jnp.logical_not(middle))
                def _():
                    ret_across(c, planes // 2 - 1, planes // 2)

            else:

                @pl.when(middle)
                def _():
                    ret_across(c, planes // 2 - 1, planes // 2)

    def take_own():
        own_all().wait_recv()
        eye = iota((req_dev, req_dev), 0) == iota((req_dev, req_dev), 1)
        for s in range(n):
            own_col[s * req_dev:(s + 1) * req_dev] = jnp.sum(
                jnp.where(eye, own_recv[s].astype(jnp.float32), 0.0), axis=1, keepdims=True
            )

    def pass_pages():
        kv_all().wait_recv()

        @pl.loop(1, n // 2)
        def _(j):
            slot = lax.rem(me + 2 * j, n)
            fw_copy(slot).start()

    def take_pages():
        fw_all().wait_recv()

    def prefix():
        tokens = n * page_len
        page = div(iota((1, tokens), 1), page_len)
        token_owner = jnp.zeros((1, tokens), jnp.float32)
        end = jnp.int32(0)
        for i in range(pc_ref.shape[0]):
            end = end + pc_ref[i]
            token_owner = token_owner + jnp.where(page >= end, 1.0, 0.0)

        block = max(32, min(rows_all, PREFIX_KI * 1024 // tokens))

        @pl.loop(0, rows_all // block)
        def _(b):
            rows = pl.ds(pl.multiple_of(b * block, block), block)
            live = own_col[rows] == token_owner
            keys = pool[:, :, :head_dim].reshape(tokens, head_dim)
            values = pool[:, :, head_dim:].reshape(tokens, head_dim)
            for h in range(per_dev):
                span = slice(h * head_dim, (h + 1) * head_dim)
                scores = lax.dot_general(
                    q_ref[rows, span], keys, (((1,), (1,)), ((), ())),
                    preferred_element_type=jnp.float32,
                )
                scores = jnp.where(live, scores, neg_large)
                top_score = jnp.max(scores, axis=1, keepdims=True)
                weight = jnp.exp2((scores - top_score) * scale)
                top[h, rows] = top_score * scale
                total[h, rows] = jnp.sum(weight, axis=1, keepdims=True)
                mix[rows, span] = jnp.dot(
                    weight.astype(jnp.bfloat16), values, preferred_element_type=jnp.float32
                )

    def factors():
        st_all().wait_recv()
        sub, lan = iota((req_dev, LANES), 0), iota((req_dev, LANES), 1)

        @pl.loop(0, n // 2)
        def _(step):
            for u in range(2):
                s = step * 2 + u
                rows = pl.ds(pl.multiple_of(s * req_dev, req_dev), req_dev)
                row = stats_recv[s]
                for h in range(per_dev):
                    span = slice(h * head_dim, (h + 1) * head_dim)
                    level = jnp.sum(
                        jnp.where(lan == h * req_dev + sub, row, 0.0), axis=1, keepdims=True
                    )
                    top_first = top[h, rows]
                    top_score = jnp.maximum(level, top_first)
                    factor_second = jnp.exp2(level - top_score)
                    factor_first = jnp.exp2(top_first - top_score)
                    inverse = 1.0 / (total[h, rows] * factor_first + factor_second)
                    mix[rows, span] = mix[rows, span] * (factor_first * inverse)
                    second_factor[rows, span] = jnp.broadcast_to(
                        factor_second * inverse, (req_dev, head_dim)
                    )

    def gather_in(c, s):
        rows = pl.ds(pl.multiple_of(s * req_dev + c * part, part), part)
        second = retrecv[c, s].astype(jnp.float32)
        out_ref[rows, :] = (mix[rows, :] + second * second_factor[rows, :]).astype(out_ref.dtype)

    def arrived(c, count, group):
        some = retrecv.at[c, pl.ds(0, count)]
        send(some, some, ret_send.at[c], ret_recv.at[c, group], partner).wait_recv()

    def gather_near(c):
        gather_in(c, me)
        arrived(c, half - 1, 0)

        @pl.loop(0, half - 1)
        def _(j):
            gather_in(c, local_of(j))

    def gather_across(c):
        if half < n:
            arrived(c, half, 1)

            @pl.loop(0, half)
            def _(j):
                gather_in(c, across_of(div(j, side), mod(j, side)))

    seen = jnp.zeros((n, LANES), jnp.float32)
    to_earlier(0)
    to_later()
    send_own()
    keep_mine()
    turn_page()
    make_orders()
    to_earlier(1)
    to_last()
    send_pages()
    suffix_in()
    q_all(0).wait_recv()
    seen = suffix(0, seen)
    send_back_near(0)
    send_back_across(0); send_back_across(0, 1)
    q_all(1).wait_recv()
    seen = suffix(1, seen)
    send_stats(seen)
    send_back_near(1)
    send_back_across(1)
    send_back_across(1, 1)
    take_own()
    pass_pages()
    take_pages()
    prefix()
    q_all(0).wait_send()
    q_all(1).wait_send()
    own_all().wait_send()
    kv_all().wait_send()
    fw_all().wait_send()
    factors()
    gather_near(0)
    gather_near(1)
    gather_across(0)
    gather_across(1)
    st_all().wait_send()
    ret_all(0).wait_send()
    ret_all(1).wait_send()


def body(queries, prefix_kv, page_counts, request_prefix, suffix_kv, suffix_len):
    n = lax.axis_size("blk")
    rows_all, width = queries.shape
    req_dev, suf_len, kv_heads, kv_width = suffix_kv.shape
    head_dim = kv_width // 2
    per_dev = width // head_dim
    page_len = prefix_kv.shape[1]
    part = req_dev // CHUNKS
    page = prefix_kv.reshape(page_len * kv_heads, kv_width)
    cache = suffix_kv.reshape(req_dev, suf_len * kv_heads, kv_width)
    bf16, f32, i32 = jnp.bfloat16, jnp.float32, jnp.int32
    dma, regular = pltpu.SemaphoreType.DMA, pltpu.SemaphoreType.REGULAR
    vmem = pl.BlockSpec(memory_space=pltpu.VMEM)
    anywhere = pl.BlockSpec(memory_space=pl.ANY)
    return pl.pallas_call(
        functools.partial(kernel, n),
        out_shape=pltpu.VMEM((rows_all, width), bf16),
        in_specs=[anywhere] * 6,
        out_specs=vmem,
        scratch_shapes=[
            pltpu.VMEM((1, req_dev), i32),
            pltpu.SMEM(page_counts.shape, i32),
            pltpu.SMEM((req_dev,), i32),
            pltpu.VMEM((rows_all, width), bf16),
            pltpu.VMEM((page_len * kv_heads, kv_width), bf16),
            pltpu.VMEM((kv_heads, page_len, kv_width), bf16),
            pltpu.VMEM((part * n, part * n), bf16),
            pltpu.VMEM((part * n, part * n), bf16),
            pltpu.VMEM((CHUNKS, n, part, width), bf16),
            pltpu.VMEM((part * n, width), bf16),
            pltpu.VMEM((part * n, width), bf16),
            pltpu.VMEM((CHUNKS, n, part, width), bf16),
            pltpu.VMEM((CHUNKS, n, part, width), bf16),
            pltpu.VMEM((n, page_len, kv_width), bf16),
            pltpu.VMEM((req_dev, suf_len * kv_heads, kv_width), bf16),
            pltpu.VMEM((n, 1, req_dev), i32),
            pltpu.VMEM((rows_all, 1), f32),
            pltpu.VMEM((n, 1, LANES), f32),
            pltpu.VMEM((n, 1, LANES), f32),
            pltpu.VMEM((rows_all, width), f32),
            pltpu.VMEM((rows_all, width), f32),
            pltpu.VMEM((per_dev, rows_all, 1), f32),
            pltpu.VMEM((per_dev, rows_all, 1), f32),
            dma((CHUNKS,)), dma((CHUNKS,)), dma, dma, dma, dma, dma, dma,
            dma((CHUNKS,)), dma((CHUNKS, 2)), dma, dma, dma, dma((5,)),
            regular((n,)),
        ],
        compiler_params=pltpu.CompilerParams(
            collective_id=0, has_side_effects=True, vmem_limit_bytes=VMEM_MIB * 1024 * 1024
        ),
    )(queries, page, request_prefix.T, page_counts, cache, suffix_len)


def solution(mesh):
    in_specs = (
        P("groups", "blk"),
        P(("groups", "blk"), None, None, None),
        P("groups"),
        P(("groups", "blk"), None),
        P(("groups", "blk"), None, None, None),
        P(("groups", "blk")),
    )
    out_specs = P("groups", "blk")
    return jax.shard_map(body, mesh=mesh, in_specs=in_specs, out_specs=out_specs, check_vma=False)
```

```python
import functools
import math

import jax
import jax.numpy as jnp
from jax import lax
from jax.experimental import pallas as pl
from jax.experimental.pallas import tpu as pltpu
from jax.sharding import PartitionSpec as P

neg_large = -1e30


def div(x, k):
    return jnp.right_shift(x, k.bit_length() - 1) if k & (k - 1) == 0 else x // k


def mod(x, k):
    return jnp.bitwise_and(x, k - 1) if k & (k - 1) == 0 else lax.rem(x, k)


MESH = pl.DeviceIdType.MESH
CHUNKS = 2
UNROLL = 8
NEAR = 1
LANES = 128
PREFIX_KI = 256
VMEM_MIB = 56
LOG2E = math.log2(math.e)


def plane_of(n):
    bits = n.bit_length() - 1
    return 1 << (bits + 1) // 2 if n & (n - 1) == 0 else 1


def kernel(
    n, q_hbm, kv_hbm, rp_hbm, pc_hbm, suf_ref, len_hbm, out_ref,
    rp_ref, pc_ref, len_ref, q_ref, kv_ref, home, order, back, qrecv, qperm, operm, retsrc, retrecv, pool, suf, own_recv,
    own_col, stats_src, stats_recv, mix, second_factor, first_level,
    q_send, q_recv_sem, own_send, own_recv_sem, kv_send, kv_recv, fw_send, fw_recv,
    ret_send, ret_recv, st_send, st_recv, suf_sem, in_sem, reply,
):
    me = lax.axis_index("blk")
    partner = me + 1 - 2 * lax.rem(me, 2)
    rows_all, width = q_ref.shape
    req_dev = rows_all // n
    part = req_dev // CHUNKS
    kv_heads, page_len, kv_width = home.shape
    head_dim = kv_width // 2
    per_dev = width // head_dim
    heads = per_dev * n
    group_size = heads // kv_heads
    share = n // kv_heads
    cols = suf_ref.shape[1]
    scale = head_dim ** -0.5 * LOG2E
    power = n & (n - 1) == 0

    def iota(shape, dim):
        return lax.broadcasted_iota(jnp.int32, shape, dim)

    def signal(sem, peer):
        pl.semaphore_signal(sem, inc=1, device_id={"blk": peer}, device_id_type=MESH)

    barrier = pltpu.get_barrier_semaphore()
    side = plane_of(n)
    planes = n // side
    plane, spot = div(me, side), mod(me, side)

    @pl.loop(me + 1, n)
    def _(p):
        signal(barrier, p)

    q_in = pltpu.make_async_copy(q_hbm, q_ref, in_sem.at[0])
    kv_in = pltpu.make_async_copy(kv_hbm, kv_ref, in_sem.at[1])
    small_in = [
        pltpu.make_async_copy(src, dst, in_sem.at[2 + i])
        for i, (src, dst) in enumerate(((rp_hbm, rp_ref), (pc_hbm, pc_ref), (len_hbm, len_ref)))
    ]
    q_in.start()
    kv_in.start()
    for copy in small_in:
        copy.start()

    def suf_copy(r):
        return pltpu.make_async_copy(suf_ref.at[r], suf.at[r], suf_sem)

    @pl.loop(0, req_dev)
    def _(r):
        suf_copy(r).start()

    def send(src, dst, s_sem, r_sem, peer):
        return pltpu.make_async_remote_copy(
            src_ref=src, dst_ref=dst, send_sem=s_sem, recv_sem=r_sem,
            device_id={"blk": peer}, device_id_type=MESH,
        )

    half = n // 2 if planes % 2 == 0 else n
    base = div(me, half) * half
    lower = me < half
    middle = (plane == planes // 2) | (plane == planes // 2 - 1)

    def peer_of(j):
        return jnp.bitwise_xor(me, j + 1) if power else lax.rem(me + j + 1, n)

    def local_of(j):
        return jnp.bitwise_xor(me, j + 1) if power else base + lax.rem(me - base + j + 1, half)

    def across_of(t, i):
        p = jnp.where(lower, planes - 1 - t, t)
        return p * side + jnp.bitwise_xor(spot, i)

    def q_copy(c, slot, peer):
        rows = pl.ds(pl.multiple_of(peer * req_dev + c * part, part), part)
        return send(q_ref.at[rows], qrecv.at[c, slot], q_send.at[c], q_recv_sem.at[c], peer)

    def q_all(c):
        some = qrecv.at[c, pl.ds(0, n - 1)]
        return send(some, some, q_send.at[c], q_recv_sem.at[c], partner)

    def own_copy(slot, peer):
        return send(rp_ref, own_recv.at[slot], own_send, own_recv_sem, peer)

    def own_all():
        some = own_recv.at[pl.ds(0, n - 1)]
        return send(some, some, own_send, own_recv_sem, partner)

    def kv_copy(slot, peer):
        return send(home.at[peer // share], pool.at[slot], kv_send, kv_recv, peer)

    def kv_all():
        some = pool.at[pl.ds(0, n // 2 - 1)]
        return send(some, some, kv_send, kv_recv, partner)

    def fw_copy(slot):
        return send(pool.at[slot], pool.at[slot], fw_send, fw_recv, partner)

    def fw_own():
        return send(home.at[me // share], pool.at[me], fw_send, fw_recv, partner)

    def fw_all():
        some = pool.at[pl.ds(0, n // 2)]
        return send(some, some, fw_send, fw_recv, partner)

    def ret_copy(c, slot, peer, group):
        return send(
            retsrc.at[c, peer], retrecv.at[c, slot], ret_send.at[c], ret_recv.at[c, group], peer
        )

    def ret_across(c, first, last):
        @pl.loop(first * side, last * side)
        def _(j):
            ret_copy(c, me, across_of(div(j, side), mod(j, side)), 1).start()

    def ret_all(c):
        some = retsrc.at[c, pl.ds(0, n - 1)]
        return send(some, some, ret_send.at[c], ret_recv.at[c, 0], partner)

    def st_copy(slot, peer):
        return send(stats_src.at[peer], stats_recv.at[slot], st_send, st_recv, peer)

    def st_all():
        some = stats_recv.at[pl.ds(0, n - 1)]
        return send(some, some, st_send, st_recv, partner)

    @pl.when(me > 0)
    def _():
        pl.semaphore_wait(barrier, me)


    @pl.loop(0, me)
    def _(j):
        signal(reply.at[me], me - 1 - j)

    q_in.wait()
    def home_plane(c, later):
        @pl.loop(1, side)
        def _(i):
            p = plane * side + jnp.bitwise_xor(spot, i)

            @pl.when(p > me if later else p < me)
            def _():
                if later and c == 0:
                    pl.semaphore_wait(reply.at[p], 1)
                q_copy(c, me, p).start()

    def to_plane(c, z, wait):
        @pl.loop(0, side)
        def _(i):
            p = z * side + jnp.bitwise_xor(spot, i)
            if wait:
                pl.semaphore_wait(reply.at[p], 1)
            q_copy(c, me, p).start()

    def to_earlier(c):
        home_plane(c, False)

        @pl.loop(0, plane)
        def _(j):
            to_plane(c, plane - 1 - j, False)

    def to_later():
        home_plane(0, True)
        home_plane(1, True)
        reach = jnp.minimum(plane + NEAR, planes)

        @pl.loop(plane + 1, reach)
        def _(z):
            to_plane(0, z, True)
            to_plane(1, z, False)

        @pl.loop(reach, planes)
        def _(z):
            to_plane(0, z, True)

    def to_last():
        @pl.loop(jnp.minimum(plane + NEAR, planes), planes)
        def _(z):
            to_plane(1, z, False)

    def send_own():
        for copy in small_in:
            copy.wait()

        @pl.loop(0, n - 1)
        def _(j):
            own_copy(me, peer_of(j)).start()

        own_recv[me] = rp_ref[...]

    def keep_mine():
        for c in range(CHUNKS):
            qrecv[c, me] = q_ref[pl.ds(pl.multiple_of(me * req_dev + c * part, part), part)]

    def turn_page():
        kv_in.wait()
        entries = kv_heads * page_len
        entry, source = iota((entries, entries), 0), iota((entries, entries), 1)
        turn = jnp.where(
            source == mod(entry, page_len) * kv_heads + div(entry, page_len), 1.0, 0.0
        ).astype(jnp.bfloat16)
        turned = jnp.dot(turn, kv_ref[...], preferred_element_type=jnp.float32)
        home[...] = turned.astype(jnp.bfloat16).reshape(home.shape)
        pool[me] = home[me // share]

    def send_pages():
        @pl.loop(1, n // 2)
        def _(j):
            kv_copy(me, lax.rem(me + 2 * j, n)).start()

        fw_own().start()

    size = part * n

    def make_orders():
        row_id, col_id = iota((size, size), 0), iota((size, size), 1)
        order[...] = jnp.where(
            col_id == mod(row_id, n) * part + div(row_id, n), 1.0, 0.0
        ).astype(jnp.bfloat16)
        back[...] = jnp.where(
            col_id == mod(row_id, part) * n + div(row_id, part), 1.0, 0.0
        ).astype(jnp.bfloat16)

    def suffix_in():
        pltpu.make_async_copy(suf_ref, suf, suf_sem).wait()

    def suffix(c, seen):
        stacked = iota((per_dev * n, cols), 0)
        head_of_row = mod(stacked, n) * per_dev + div(stacked, n)
        column = iota((per_dev * n, cols), 1)
        own_kv = div(head_of_row, group_size) == mod(column, kv_heads)
        position = jnp.where(own_kv, div(column, kv_heads), cols)
        lane = iota((n, LANES), 1)
        qperm[...] = jnp.dot(
            order[...], qrecv[c].reshape(size, width), preferred_element_type=jnp.float32
        ).astype(jnp.bfloat16)

        def some_requests(step, seen):
            ids = [step * UNROLL + u for u in range(UNROLL)]
            all_scores = []
            for local in ids:
                rows = pl.ds(pl.multiple_of(local * n, n), n)
                qr = jnp.concatenate(
                    [qperm[rows, h * head_dim:(h + 1) * head_dim] for h in range(per_dev)], axis=0
                )
                all_scores.append(lax.dot_general(
                    qr, suf[c * part + local, :, :head_dim], (((1,), (1,)), ((), ())),
                    preferred_element_type=jnp.float32,
                ))
            for local, scores in zip(ids, all_scores):
                r = c * part + local
                rows = pl.ds(pl.multiple_of(local * n, n), n)
                scores = jnp.where(position < len_ref[r], scores, neg_large)
                top_score = jnp.max(scores, axis=1, keepdims=True)
                weight = jnp.exp2((scores - top_score) * scale)
                weight_sum = jnp.sum(weight, axis=1, keepdims=True)
                mixed = jnp.dot(
                    weight.astype(jnp.bfloat16), suf[r, :, head_dim:],
                    preferred_element_type=jnp.float32,
                )
                result = (mixed * (1.0 / weight_sum)).astype(jnp.bfloat16)
                level = top_score * scale + jnp.log(weight_sum) * LOG2E
                for h in range(per_dev):
                    operm[rows, h * head_dim:(h + 1) * head_dim] = result[h * n:(h + 1) * n]
                    seen = jnp.where(
                        lane == h * req_dev + r, level[h * n:(h + 1) * n], seen
                    )
            return seen

        seen = lax.fori_loop(0, part // UNROLL, some_requests, seen)
        returned = jnp.dot(back[...], operm[...], preferred_element_type=jnp.float32)
        retsrc[c] = returned.astype(jnp.bfloat16).reshape(n, part, width)
        retrecv[c, me] = retsrc[c, me]
        return seen

    def send_stats(seen):
        for p in range(n):
            stats_src[p] = seen[p:p + 1, :]

        @pl.loop(0, n - 1)
        def _(j):
            st_copy(me, peer_of(j)).start()

        stats_recv[me] = stats_src[me]

    def send_back_near(c):
        @pl.loop(0, half - 1)
        def _(j):
            ret_copy(c, me, local_of(j), 0).start()

    def send_back_across(c, part=0):
        if half < n:
            if part == 0:
                ret_across(c, 0, planes // 2 - 1)

                @pl.when(jnp.logical_not(middle))
                def _():
                    ret_across(c, planes // 2 - 1, planes // 2)

            else:

                @pl.when(middle)
                def _():
                    ret_across(c, planes // 2 - 1, planes // 2)

    def take_own():
        own_all().wait_recv()
        eye = iota((req_dev, req_dev), 0) == iota((req_dev, req_dev), 1)
        for s in range(n):
            own_col[s * req_dev:(s + 1) * req_dev] = jnp.sum(
                jnp.where(eye, own_recv[s].astype(jnp.float32), 0.0), axis=1, keepdims=True
            )

    def pass_pages():
        kv_all().wait_recv()

        @pl.loop(1, n // 2)
        def _(j):
            slot = lax.rem(me + 2 * j, n)
            fw_copy(slot).start()

    def take_pages():
        fw_all().wait_recv()

    def prefix():
        tokens = n * page_len
        page = div(iota((1, tokens), 1), page_len)
        token_owner = jnp.zeros((1, tokens), jnp.float32)
        end = jnp.int32(0)
        for i in range(pc_ref.shape[0]):
            end = end + pc_ref[i]
            token_owner = token_owner + jnp.where(page >= end, 1.0, 0.0)

        block = max(32, min(rows_all, PREFIX_KI * 1024 // tokens))

        @pl.loop(0, rows_all // block)
        def _(b):
            rows = pl.ds(pl.multiple_of(b * block, block), block)
            live = own_col[rows] == token_owner
            keys = pool[:, :, :head_dim].reshape(tokens, head_dim)
            values = pool[:, :, head_dim:].reshape(tokens, head_dim)
            for h in range(per_dev):
                span = slice(h * head_dim, (h + 1) * head_dim)
                scores = lax.dot_general(
                    q_ref[rows, span], keys, (((1,), (1,)), ((), ())),
                    preferred_element_type=jnp.float32,
                )
                scores = jnp.where(live, scores, neg_large)
                top_score = jnp.max(scores, axis=1, keepdims=True)
                weight = jnp.exp2((scores - top_score) * scale)
                weight_sum = jnp.sum(weight, axis=1, keepdims=True)
                first_level[h, rows] = top_score * scale + jnp.log(weight_sum) * LOG2E
                mix[rows, span] = jnp.dot(
                    weight.astype(jnp.bfloat16), values, preferred_element_type=jnp.float32
                ) * (1.0 / weight_sum)

    def factors():
        st_all().wait_recv()
        sub, lan = iota((req_dev, LANES), 0), iota((req_dev, LANES), 1)

        @pl.loop(0, n // 2)
        def _(step):
            for u in range(2):
                s = step * 2 + u
                rows = pl.ds(pl.multiple_of(s * req_dev, req_dev), req_dev)
                row = stats_recv[s]
                for h in range(per_dev):
                    span = slice(h * head_dim, (h + 1) * head_dim)
                    level = jnp.sum(
                        jnp.where(lan == h * req_dev + sub, row, 0.0), axis=1, keepdims=True
                    )
                    share_of_second = 1.0 / (1.0 + jnp.exp2(first_level[h, rows] - level))
                    second_factor[rows, span] = jnp.broadcast_to(
                        share_of_second, (req_dev, head_dim)
                    )

    def gather_in(c, s):
        rows = pl.ds(pl.multiple_of(s * req_dev + c * part, part), part)
        second = retrecv[c, s].astype(jnp.float32)
        first = mix[rows, :]
        mixed = first + (second - first) * second_factor[rows, :]
        out_ref[rows, :] = mixed.astype(out_ref.dtype)

    def arrived(c, count, group):
        some = retrecv.at[c, pl.ds(0, count)]
        send(some, some, ret_send.at[c], ret_recv.at[c, group], partner).wait_recv()

    def gather_near(c):
        gather_in(c, me)
        arrived(c, half - 1, 0)

        @pl.loop(0, half - 1)
        def _(j):
            gather_in(c, local_of(j))

    def gather_across(c):
        if half < n:
            arrived(c, half, 1)

            @pl.loop(0, half)
            def _(j):
                gather_in(c, across_of(div(j, side), mod(j, side)))

    seen = jnp.zeros((n, LANES), jnp.float32)
    to_earlier(0)
    to_later()
    send_own()
    keep_mine()
    turn_page()
    make_orders()
    q_all(0).wait_send()
    to_earlier(1)
    to_last()
    send_pages()
    suffix_in()
    q_all(0).wait_recv()
    seen = suffix(0, seen)
    send_back_near(0)
    send_back_across(0); send_back_across(0, 1)
    q_all(1).wait_recv()
    seen = suffix(1, seen)
    send_stats(seen)
    send_back_near(1)
    send_back_across(1)
    send_back_across(1, 1)
    take_own()
    pass_pages()
    take_pages()
    prefix()
    q_all(1).wait_send()
    kv_all().wait_send()
    own_all().wait_send()
    fw_all().wait_send()
    factors()
    gather_near(0)
    gather_near(1)
    gather_across(0)
    gather_across(1)
    st_all().wait_send()
    ret_all(0).wait_send()
    ret_all(1).wait_send()


def body(queries, prefix_kv, page_counts, request_prefix, suffix_kv, suffix_len):
    n = lax.axis_size("blk")
    rows_all, width = queries.shape
    req_dev, suf_len, kv_heads, kv_width = suffix_kv.shape
    head_dim = kv_width // 2
    per_dev = width // head_dim
    page_len = prefix_kv.shape[1]
    part = req_dev // CHUNKS
    page = prefix_kv.reshape(page_len * kv_heads, kv_width)
    cache = suffix_kv.reshape(req_dev, suf_len * kv_heads, kv_width)
    bf16, f32, i32 = jnp.bfloat16, jnp.float32, jnp.int32
    dma, regular = pltpu.SemaphoreType.DMA, pltpu.SemaphoreType.REGULAR
    vmem = pl.BlockSpec(memory_space=pltpu.VMEM)
    anywhere = pl.BlockSpec(memory_space=pl.ANY)
    return pl.pallas_call(
        functools.partial(kernel, n),
        out_shape=pltpu.VMEM((rows_all, width), bf16),
        in_specs=[anywhere] * 6,
        out_specs=vmem,
        scratch_shapes=[
            pltpu.VMEM((1, req_dev), i32),
            pltpu.SMEM(page_counts.shape, i32),
            pltpu.SMEM((req_dev,), i32),
            pltpu.VMEM((rows_all, width), bf16),
            pltpu.VMEM((page_len * kv_heads, kv_width), bf16),
            pltpu.VMEM((kv_heads, page_len, kv_width), bf16),
            pltpu.VMEM((part * n, part * n), bf16),
            pltpu.VMEM((part * n, part * n), bf16),
            pltpu.VMEM((CHUNKS, n, part, width), bf16),
            pltpu.VMEM((part * n, width), bf16),
            pltpu.VMEM((part * n, width), bf16),
            pltpu.VMEM((CHUNKS, n, part, width), bf16),
            pltpu.VMEM((CHUNKS, n, part, width), bf16),
            pltpu.VMEM((n, page_len, kv_width), bf16),
            pltpu.VMEM((req_dev, suf_len * kv_heads, kv_width), bf16),
            pltpu.VMEM((n, 1, req_dev), i32),
            pltpu.VMEM((rows_all, 1), f32),
            pltpu.VMEM((n, 1, LANES), f32),
            pltpu.VMEM((n, 1, LANES), f32),
            pltpu.VMEM((rows_all, width), f32),
            pltpu.VMEM((rows_all, width), f32),
            pltpu.VMEM((per_dev, rows_all, 1), f32),
            dma((CHUNKS,)), dma((CHUNKS,)), dma, dma, dma, dma, dma, dma,
            dma((CHUNKS,)), dma((CHUNKS, 2)), dma, dma, dma, dma((5,)),
            regular((n,)),
        ],
        compiler_params=pltpu.CompilerParams(
            collective_id=0, has_side_effects=True, vmem_limit_bytes=VMEM_MIB * 1024 * 1024
        ),
    )(queries, page, request_prefix.T, page_counts, cache, suffix_len)


def solution(mesh):
    in_specs = (
        P("groups", "blk"),
        P(("groups", "blk"), None, None, None),
        P("groups"),
        P(("groups", "blk"), None),
        P(("groups", "blk"), None, None, None),
        P(("groups", "blk")),
    )
    out_specs = P("groups", "blk")
    return jax.shard_map(body, mesh=mesh, in_specs=in_specs, out_specs=out_specs, check_vma=False)
```

```python
import functools
import math

import jax
import jax.numpy as jnp
from jax import lax
from jax.experimental import pallas as pl
from jax.experimental.pallas import tpu as pltpu
from jax.sharding import PartitionSpec as P

neg_large = -1e30


def div(x, k):
    return jnp.right_shift(x, k.bit_length() - 1) if k & (k - 1) == 0 else x // k


def mod(x, k):
    return jnp.bitwise_and(x, k - 1) if k & (k - 1) == 0 else lax.rem(x, k)


MESH = pl.DeviceIdType.MESH
CHUNKS = 2
UNROLL = 8
NEAR = 1
LANES = 128
PREFIX_KI = 256
VMEM_MIB = 56
LOG2E = math.log2(math.e)


def plane_of(n):
    bits = n.bit_length() - 1
    return 1 << (bits + 1) // 2 if n & (n - 1) == 0 else 1


def kernel(
    n, q_hbm, kv_hbm, rp_hbm, pc_hbm, suf_ref, len_hbm, out_ref,
    rp_ref, pc_ref, len_ref, q_ref, kv_ref, home, order, back, qrecv, qperm, operm, retsrc, retrecv, pool, suf, own_recv,
    own_col, stats_src, stats_recv, mix, second_factor, first_level,
    q_send, q_recv_sem, own_send, own_recv_sem, kv_send, kv_recv, fw_send, fw_recv,
    ret_send, ret_recv, st_send, st_recv, suf_sem, in_sem, reply,
):
    me = lax.axis_index("blk")
    partner = me + 1 - 2 * lax.rem(me, 2)
    rows_all, width = q_ref.shape
    req_dev = rows_all // n
    part = req_dev // CHUNKS
    kv_heads, page_len, kv_width = home.shape
    head_dim = kv_width // 2
    per_dev = width // head_dim
    heads = per_dev * n
    group_size = heads // kv_heads
    share = n // kv_heads
    cols = suf_ref.shape[1]
    scale = head_dim ** -0.5 * LOG2E
    power = n & (n - 1) == 0

    def iota(shape, dim):
        return lax.broadcasted_iota(jnp.int32, shape, dim)

    def signal(sem, peer):
        pl.semaphore_signal(sem, inc=1, device_id={"blk": peer}, device_id_type=MESH)

    barrier = pltpu.get_barrier_semaphore()
    side = plane_of(n)
    planes = n // side
    plane, spot = div(me, side), mod(me, side)

    @pl.loop(me + 1, n)
    def _(p):
        signal(barrier, p)

    q_in = pltpu.make_async_copy(q_hbm, q_ref, in_sem.at[0])
    kv_in = pltpu.make_async_copy(kv_hbm, kv_ref, in_sem.at[1])
    small_in = [
        pltpu.make_async_copy(src, dst, in_sem.at[2 + i])
        for i, (src, dst) in enumerate(((rp_hbm, rp_ref), (pc_hbm, pc_ref), (len_hbm, len_ref)))
    ]
    q_in.start()
    kv_in.start()
    for copy in small_in:
        copy.start()

    def suf_copy(r):
        return pltpu.make_async_copy(suf_ref.at[r], suf.at[r], suf_sem)

    @pl.loop(0, req_dev)
    def _(r):
        suf_copy(r).start()

    def send(src, dst, s_sem, r_sem, peer):
        return pltpu.make_async_remote_copy(
            src_ref=src, dst_ref=dst, send_sem=s_sem, recv_sem=r_sem,
            device_id={"blk": peer}, device_id_type=MESH,
        )

    half = n // 2 if planes % 2 == 0 else n
    base = div(me, half) * half
    lower = me < half
    middle = (plane == planes // 2) | (plane == planes // 2 - 1)

    def peer_of(j):
        return jnp.bitwise_xor(me, j + 1) if power else lax.rem(me + j + 1, n)

    def local_of(j):
        return jnp.bitwise_xor(me, j + 1) if power else base + lax.rem(me - base + j + 1, half)

    def across_of(t, i):
        p = jnp.where(lower, planes - 1 - t, t)
        return p * side + jnp.bitwise_xor(spot, i)

    def q_copy(c, slot, peer):
        rows = pl.ds(pl.multiple_of(peer * req_dev + c * part, part), part)
        return send(q_ref.at[rows], qrecv.at[c, slot], q_send.at[c], q_recv_sem.at[c], peer)

    def q_all(c):
        some = qrecv.at[c, pl.ds(0, n - 1)]
        return send(some, some, q_send.at[c], q_recv_sem.at[c], partner)

    def own_copy(slot, peer):
        return send(rp_ref, own_recv.at[slot], own_send, own_recv_sem, peer)

    def own_all():
        some = own_recv.at[pl.ds(0, n - 1)]
        return send(some, some, own_send, own_recv_sem, partner)

    def kv_copy(slot, peer):
        return send(home.at[peer // share], pool.at[slot], kv_send, kv_recv, peer)

    def kv_all():
        some = pool.at[pl.ds(0, n // 2 - 1)]
        return send(some, some, kv_send, kv_recv, partner)

    def fw_copy(slot):
        return send(pool.at[slot], pool.at[slot], fw_send, fw_recv, partner)

    def fw_own():
        return send(home.at[me // share], pool.at[me], fw_send, fw_recv, partner)

    def fw_all():
        some = pool.at[pl.ds(0, n // 2)]
        return send(some, some, fw_send, fw_recv, partner)

    def ret_copy(c, slot, peer, group):
        return send(
            retsrc.at[c, peer], retrecv.at[c, slot], ret_send.at[c], ret_recv.at[c, group], peer
        )

    def ret_across(c, first, last):
        @pl.loop(first * side, last * side)
        def _(j):
            ret_copy(c, me, across_of(div(j, side), mod(j, side)), 1).start()

    def ret_all(c):
        some = retsrc.at[c, pl.ds(0, n - 1)]
        return send(some, some, ret_send.at[c], ret_recv.at[c, 0], partner)

    def st_copy(slot, peer):
        return send(stats_src.at[peer], stats_recv.at[slot], st_send, st_recv, peer)

    def st_all():
        some = stats_recv.at[pl.ds(0, n - 1)]
        return send(some, some, st_send, st_recv, partner)

    @pl.when(me > 0)
    def _():
        pl.semaphore_wait(barrier, me)


    @pl.loop(0, me)
    def _(j):
        signal(reply.at[me], me - 1 - j)

    q_in.wait()
    def home_plane(c, later):
        @pl.loop(1, side)
        def _(i):
            p = plane * side + jnp.bitwise_xor(spot, i)

            @pl.when(p > me if later else p < me)
            def _():
                if later and c == 0:
                    pl.semaphore_wait(reply.at[p], 1)
                q_copy(c, me, p).start()

    def to_plane(c, z, wait):
        @pl.loop(0, side)
        def _(i):
            p = z * side + jnp.bitwise_xor(spot, i)
            if wait:
                pl.semaphore_wait(reply.at[p], 1)
            q_copy(c, me, p).start()

    def to_earlier(c):
        home_plane(c, False)

        @pl.loop(0, plane)
        def _(j):
            to_plane(c, plane - 1 - j, False)

    def to_later():
        home_plane(0, True)
        home_plane(1, True)
        reach = jnp.minimum(plane + NEAR, planes)

        @pl.loop(plane + 1, reach)
        def _(z):
            to_plane(0, z, True)
            to_plane(1, z, False)

        @pl.loop(reach, planes)
        def _(z):
            to_plane(0, z, True)

    def to_last():
        @pl.loop(jnp.minimum(plane + NEAR, planes), planes)
        def _(z):
            to_plane(1, z, False)

    def send_own():
        for copy in small_in:
            copy.wait()

        @pl.loop(0, n - 1)
        def _(j):
            own_copy(me, peer_of(j)).start()

        own_recv[me] = rp_ref[...]

    def keep_mine():
        for c in range(CHUNKS):
            qrecv[c, me] = q_ref[pl.ds(pl.multiple_of(me * req_dev + c * part, part), part)]

    def turn_page():
        kv_in.wait()
        entries = kv_heads * page_len
        entry, source = iota((entries, entries), 0), iota((entries, entries), 1)
        turn = jnp.where(
            source == mod(entry, page_len) * kv_heads + div(entry, page_len), 1.0, 0.0
        ).astype(jnp.bfloat16)
        turned = jnp.dot(turn, kv_ref[...], preferred_element_type=jnp.float32)
        home[...] = turned.astype(jnp.bfloat16).reshape(home.shape)
        pool[me] = home[me // share]

    def send_pages():
        @pl.loop(1, n // 2)
        def _(j):
            kv_copy(me, lax.rem(me + 2 * j, n)).start()

        fw_own().start()

    size = part * n

    def make_orders():
        row_id, col_id = iota((size, size), 0), iota((size, size), 1)
        order[...] = jnp.where(
            col_id == mod(row_id, n) * part + div(row_id, n), 1.0, 0.0
        ).astype(jnp.bfloat16)
        back[...] = jnp.where(
            col_id == mod(row_id, part) * n + div(row_id, part), 1.0, 0.0
        ).astype(jnp.bfloat16)

    def suffix_in():
        pltpu.make_async_copy(suf_ref, suf, suf_sem).wait()

    def send_stats(seen):
        for p in range(n):
            stats_src[p] = seen[p:p + 1, :]

        @pl.loop(0, n - 1)
        def _(j):
            st_copy(me, peer_of(j)).start()

        stats_recv[me] = stats_src[me]

    def suffix(c, seen):
        stacked = iota((per_dev * n, cols), 0)
        head_of_row = mod(stacked, n) * per_dev + div(stacked, n)
        column = iota((per_dev * n, cols), 1)
        own_kv = div(head_of_row, group_size) == mod(column, kv_heads)
        position = jnp.where(own_kv, div(column, kv_heads), cols)
        lane = iota((n, LANES), 1)
        qperm[...] = jnp.dot(
            order[...], qrecv[c].reshape(size, width), preferred_element_type=jnp.float32
        ).astype(jnp.bfloat16)

        def some_requests(step, seen):
            ids = [step * UNROLL + u for u in range(UNROLL)]
            all_scores = []
            for local in ids:
                rows = pl.ds(pl.multiple_of(local * n, n), n)
                qr = jnp.concatenate(
                    [qperm[rows, h * head_dim:(h + 1) * head_dim] for h in range(per_dev)], axis=0
                )
                all_scores.append(lax.dot_general(
                    qr, suf[c * part + local, :, :head_dim], (((1,), (1,)), ((), ())),
                    preferred_element_type=jnp.float32,
                ))
            for local, scores in zip(ids, all_scores):
                r = c * part + local
                rows = pl.ds(pl.multiple_of(local * n, n), n)
                scores = jnp.where(position < len_ref[r], scores, neg_large)
                top_score = jnp.max(scores, axis=1, keepdims=True)
                weight = jnp.exp2((scores - top_score) * scale)
                weight_sum = jnp.sum(weight, axis=1, keepdims=True)
                mixed = jnp.dot(
                    weight.astype(jnp.bfloat16), suf[r, :, head_dim:],
                    preferred_element_type=jnp.float32,
                )
                result = (mixed * (1.0 / weight_sum)).astype(jnp.bfloat16)
                level = top_score * scale + jnp.log(weight_sum) * LOG2E
                for h in range(per_dev):
                    operm[rows, h * head_dim:(h + 1) * head_dim] = result[h * n:(h + 1) * n]
                    seen = jnp.where(
                        lane == h * req_dev + r, level[h * n:(h + 1) * n], seen
                    )
            return seen

        seen = lax.fori_loop(0, part // UNROLL, some_requests, seen)
        if c == CHUNKS - 1:
            send_stats(seen)
        returned = jnp.dot(back[...], operm[...], preferred_element_type=jnp.float32)
        retsrc[c] = returned.astype(jnp.bfloat16).reshape(n, part, width)
        retrecv[c, me] = retsrc[c, me]
        return seen

    def send_back_near(c):
        @pl.loop(0, half - 1)
        def _(j):
            ret_copy(c, me, local_of(j), 0).start()

    def send_back_across(c, part=0):
        if half < n:
            if part == 0:
                ret_across(c, 0, planes // 2 - 1)

                @pl.when(jnp.logical_not(middle))
                def _():
                    ret_across(c, planes // 2 - 1, planes // 2)

            else:

                @pl.when(middle)
                def _():
                    ret_across(c, planes // 2 - 1, planes // 2)

    def take_own():
        own_all().wait_recv()
        eye = iota((req_dev, req_dev), 0) == iota((req_dev, req_dev), 1)
        for s in range(n):
            own_col[s * req_dev:(s + 1) * req_dev] = jnp.sum(
                jnp.where(eye, own_recv[s].astype(jnp.float32), 0.0), axis=1, keepdims=True
            )

    def pass_pages():
        kv_all().wait_recv()

        @pl.loop(1, n // 2)
        def _(j):
            slot = lax.rem(me + 2 * j, n)
            fw_copy(slot).start()

    def take_pages():
        fw_all().wait_recv()

    def prefix():
        tokens = n * page_len
        page = div(iota((1, tokens), 1), page_len)
        token_owner = jnp.zeros((1, tokens), jnp.float32)
        end = jnp.int32(0)
        for i in range(pc_ref.shape[0]):
            end = end + pc_ref[i]
            token_owner = token_owner + jnp.where(page >= end, 1.0, 0.0)

        block = max(32, min(rows_all, PREFIX_KI * 1024 // tokens))

        @pl.loop(0, rows_all // block)
        def _(b):
            rows = pl.ds(pl.multiple_of(b * block, block), block)
            live = own_col[rows] == token_owner
            keys = pool[:, :, :head_dim].reshape(tokens, head_dim)
            values = pool[:, :, head_dim:].reshape(tokens, head_dim)
            for h in range(per_dev):
                span = slice(h * head_dim, (h + 1) * head_dim)
                scores = lax.dot_general(
                    q_ref[rows, span], keys, (((1,), (1,)), ((), ())),
                    preferred_element_type=jnp.float32,
                )
                scores = jnp.where(live, scores, neg_large)
                top_score = jnp.max(scores, axis=1, keepdims=True)
                weight = jnp.exp2((scores - top_score) * scale)
                weight_sum = jnp.sum(weight, axis=1, keepdims=True)
                first_level[h, rows] = top_score * scale + jnp.log(weight_sum) * LOG2E
                mix[rows, span] = jnp.dot(
                    weight.astype(jnp.bfloat16), values, preferred_element_type=jnp.float32
                ) * (1.0 / weight_sum)

    def factors():
        st_all().wait_recv()
        sub, lan = iota((req_dev, LANES), 0), iota((req_dev, LANES), 1)

        @pl.loop(0, n // 2)
        def _(step):
            for u in range(2):
                s = step * 2 + u
                rows = pl.ds(pl.multiple_of(s * req_dev, req_dev), req_dev)
                row = stats_recv[s]
                for h in range(per_dev):
                    span = slice(h * head_dim, (h + 1) * head_dim)
                    level = jnp.sum(
                        jnp.where(lan == h * req_dev + sub, row, 0.0), axis=1, keepdims=True
                    )
                    share_of_second = 1.0 / (1.0 + jnp.exp2(first_level[h, rows] - level))
                    second_factor[rows, span] = jnp.broadcast_to(
                        share_of_second, (req_dev, head_dim)
                    )

    def gather_in(c, s):
        rows = pl.ds(pl.multiple_of(s * req_dev + c * part, part), part)
        second = retrecv[c, s].astype(jnp.float32)
        first = mix[rows, :]
        mixed = first + (second - first) * second_factor[rows, :]
        out_ref[rows, :] = mixed.astype(out_ref.dtype)

    def arrived(c, count, group):
        some = retrecv.at[c, pl.ds(0, count)]
        send(some, some, ret_send.at[c], ret_recv.at[c, group], partner).wait_recv()

    def gather_near(c):
        gather_in(c, me)
        arrived(c, half - 1, 0)

        @pl.loop(0, half - 1)
        def _(j):
            gather_in(c, local_of(j))

    def gather_across(c):
        if half < n:
            arrived(c, half, 1)

            @pl.loop(0, half)
            def _(j):
                gather_in(c, across_of(div(j, side), mod(j, side)))

    seen = jnp.zeros((n, LANES), jnp.float32)
    to_earlier(0)
    to_later()
    send_own()
    keep_mine()
    turn_page()
    make_orders()
    q_all(0).wait_send()
    to_earlier(1)
    to_last()
    send_pages()
    suffix_in()
    q_all(0).wait_recv()
    seen = suffix(0, seen)
    send_back_near(0)
    send_back_across(0); send_back_across(0, 1)
    q_all(1).wait_recv()
    seen = suffix(1, seen)
    pass
    send_back_near(1)
    send_back_across(1)
    send_back_across(1, 1)
    take_own()
    pass_pages()
    take_pages()
    prefix()
    q_all(1).wait_send()
    kv_all().wait_send()
    own_all().wait_send()
    fw_all().wait_send()
    factors()
    gather_near(0)
    gather_near(1)
    gather_across(0)
    gather_across(1)
    st_all().wait_send()
    ret_all(0).wait_send()
    ret_all(1).wait_send()


def body(queries, prefix_kv, page_counts, request_prefix, suffix_kv, suffix_len):
    n = lax.axis_size("blk")
    rows_all, width = queries.shape
    req_dev, suf_len, kv_heads, kv_width = suffix_kv.shape
    head_dim = kv_width // 2
    per_dev = width // head_dim
    page_len = prefix_kv.shape[1]
    part = req_dev // CHUNKS
    page = prefix_kv.reshape(page_len * kv_heads, kv_width)
    cache = suffix_kv.reshape(req_dev, suf_len * kv_heads, kv_width)
    bf16, f32, i32 = jnp.bfloat16, jnp.float32, jnp.int32
    dma, regular = pltpu.SemaphoreType.DMA, pltpu.SemaphoreType.REGULAR
    vmem = pl.BlockSpec(memory_space=pltpu.VMEM)
    anywhere = pl.BlockSpec(memory_space=pl.ANY)
    return pl.pallas_call(
        functools.partial(kernel, n),
        out_shape=pltpu.VMEM((rows_all, width), bf16),
        in_specs=[anywhere] * 6,
        out_specs=vmem,
        scratch_shapes=[
            pltpu.VMEM((1, req_dev), i32),
            pltpu.SMEM(page_counts.shape, i32),
            pltpu.SMEM((req_dev,), i32),
            pltpu.VMEM((rows_all, width), bf16),
            pltpu.VMEM((page_len * kv_heads, kv_width), bf16),
            pltpu.VMEM((kv_heads, page_len, kv_width), bf16),
            pltpu.VMEM((part * n, part * n), bf16),
            pltpu.VMEM((part * n, part * n), bf16),
            pltpu.VMEM((CHUNKS, n, part, width), bf16),
            pltpu.VMEM((part * n, width), bf16),
            pltpu.VMEM((part * n, width), bf16),
            pltpu.VMEM((CHUNKS, n, part, width), bf16),
            pltpu.VMEM((CHUNKS, n, part, width), bf16),
            pltpu.VMEM((n, page_len, kv_width), bf16),
            pltpu.VMEM((req_dev, suf_len * kv_heads, kv_width), bf16),
            pltpu.VMEM((n, 1, req_dev), i32),
            pltpu.VMEM((rows_all, 1), f32),
            pltpu.VMEM((n, 1, LANES), f32),
            pltpu.VMEM((n, 1, LANES), f32),
            pltpu.VMEM((rows_all, width), f32),
            pltpu.VMEM((rows_all, width), f32),
            pltpu.VMEM((per_dev, rows_all, 1), f32),
            dma((CHUNKS,)), dma((CHUNKS,)), dma, dma, dma, dma, dma, dma,
            dma((CHUNKS,)), dma((CHUNKS, 2)), dma, dma, dma, dma((5,)),
            regular((n,)),
        ],
        compiler_params=pltpu.CompilerParams(
            collective_id=0, has_side_effects=True, vmem_limit_bytes=VMEM_MIB * 1024 * 1024
        ),
    )(queries, page, request_prefix.T, page_counts, cache, suffix_len)


def solution(mesh):
    in_specs = (
        P("groups", "blk"),
        P(("groups", "blk"), None, None, None),
        P("groups"),
        P(("groups", "blk"), None),
        P(("groups", "blk"), None, None, None),
        P(("groups", "blk")),
    )
    out_specs = P("groups", "blk")
    return jax.shard_map(body, mesh=mesh, in_specs=in_specs, out_specs=out_specs, check_vma=False)
```
